512 devices in a mesh: dp: 64 (over y_lo, z, core), mp: 8 (over y_hi, x).
Axes of the slice: x: 4, y: 4 (y_hi: 2, y_lo: 2; y = y_hi * 2 + y_lo), z: 16, core: 2. Of those that a mesh axis runs over, the one named last changes fastest.
Arguments:
- hidden_in: bfloat16 [32768, 4096], P('dp'), may hold values from -1.5 to 1.5
- w_query: bfloat16 [4096, 4096], P('dp', 'mp'), may hold values from -1 to 1
- w_key: bfloat16 [4096, 1024], P('dp', 'mp'), may hold values from -24 to 24
- w_value: bfloat16 [4096, 1024], P('dp', 'mp'), may hold values from -1 to 1
- w_out: bfloat16 [4096, 4096], P('dp', 'mp'), may hold values from -1 to 1
- value_weight: float32 [4096], P('mp'), may hold values from -0.09375 to 0.09375
- rewards: float32 [32768], P('dp'), may hold values from -0.6 to 0.6
- old_values: float32 [32768], P('dp'), may hold values from -6 to 6
- lengths: int32 [256], replicated, may hold values from 1 to 2048, 32768 in all
- terminal: int32 [256], replicated, may hold values 0 or 1
Outputs:
- value: float32 [32768], P('dp')
- advantage: float32 [32768], P('dp')
- value_loss: float32 [], replicated
The draws below stay inside these ranges and needn't reach their ends.
All inputs are finite; a program needn't handle non-finite values.
Results may differ from the reference program's by a relative error of at most 0.012.
The reference program's roundings to bfloat16 on the way (of `normed`, `values_proj`, `probs` and `attended`) count: a program that leaves them out, or rounds other values in their place, can miss the bound.
Values may be sent and summed in bfloat16 or wider, within the bound.
A program may use at most 128 MiB of HBM per device.

```python
import math
import jax
import jax.numpy as jnp
import numpy as np
from jax import lax

D = 4096
HEADS = 32
KV_HEADS = 8
HEAD = 128
TOK_DEV = 512
MAX_LEN = 2048
EPISODES = 256
TOKENS = 32768
N_DP = 64


def shared_query(key):
    base = jax.random.fold_in(key, 11)
    sample = jnp.clip(jax.random.normal(base, (D, HEADS * HEAD), jnp.float32), -4.0, 4.0)
    return sample * D ** (-0.5)


def mixed_blocks(key, common_shape, full_shape):
    common_key = jax.random.fold_in(key, 1)
    private_key = jax.random.fold_in(key, 2)
    common = jnp.clip(jax.random.normal(common_key, common_shape, jnp.float32), -4.0, 4.0)
    private = jnp.clip(jax.random.normal(private_key, full_shape, jnp.float32), -4.0, 4.0)
    return 0.8 * common + 0.6 * private


def draw_w_query(key, part):
    return shared_query(key).astype(jnp.bfloat16)


def draw_w_key(key, part):
    noise = jnp.clip(jax.random.normal(jax.random.fold_in(key, 23), (D, KV_HEADS * HEAD), jnp.float32), -4.0, 4.0) * D ** (-0.5)
    return noise.astype(jnp.bfloat16)


def draw_w_value(key, part):
    sample = mixed_blocks(jax.random.fold_in(key, 51), (D, 1, HEAD), (D, KV_HEADS, HEAD))
    return (sample.reshape(D, KV_HEADS * HEAD) * D ** (-0.5)).astype(jnp.bfloat16)


def draw_w_out(key, part):
    sample = mixed_blocks(jax.random.fold_in(key, 67), (1, HEAD, D), (HEADS, HEAD, D))
    return (sample.reshape(HEADS * HEAD, D) * (HEADS * HEAD) ** (-0.5)).astype(jnp.bfloat16)


def touch_ends(result, own_key, least, high):
    extent = result.shape
    spot = [jax.random.randint(jax.random.fold_in(own_key, axis), (), 0, extent[axis]) for axis in range(len(extent))]
    result = result.at[tuple(spot)].set(least)
    longest = extent.index(max(extent))
    spot[longest] = (spot[longest] + 1) % extent[longest]
    return result.at[tuple(spot)].set(high)


def block_scale(rng, extent, shards, low, high):
    def one(dim, parts):
        steps = jax.random.uniform(jax.random.fold_in(jax.random.fold_in(rng, 6), dim), (parts,), jnp.float32, low / len(shards), high / len(shards))
        return jnp.repeat(jnp.exp(steps), extent[dim] // parts).reshape((-1,) + (1,) * (len(extent) - dim - 1))

    level = one(*shards[0])
    for cut in shards[1:]:
        level = level * one(*cut)
    return level


def profile(amount, total, limit, lean):
    portions = [(1 << 20) // math.isqrt(rank ** lean) + 1 for rank in range(2, amount + 1)]
    rest, given = total - limit - (amount - 1), [1] * (amount - 1)
    while rest > 0:
        candidates = [i for i in range(amount - 1) if given[i] < limit]
        pool, left = sum([portions[i] for i in candidates]), rest
        for i in candidates:
            extra = min(limit - given[i], max(1, left * portions[i] // pool), rest)
            given[i] = given[i] + extra
            rest = rest - extra
    return np.array([limit] + given)


def ragged_sizes(rng, number_of, total, reach, lean):
    if number_of == 2:
        one = jax.random.randint(rng, (), max(1, total - reach), min(reach, total - 1) + 1)
        return jnp.stack([one, total - one])
    tallies = jnp.asarray(profile(number_of, total, reach, lean), jnp.int32)
    couples = (number_of - 1) // 2
    giver, sink = tallies[1:1 + 2 * couples:2], tallies[2:2 + 2 * couples:2]
    slack = jnp.minimum(giver - 1, reach - sink)
    moved = jax.random.randint(jax.random.fold_in(rng, 1), (couples,), 0, 1 << 20) % (slack + 1)
    tallies = tallies.at[1:1 + 2 * couples:2].set(giver - moved).at[2:2 + 2 * couples:2].set(sink + moved)
    return tallies[jax.random.permutation(jax.random.fold_in(rng, 2), number_of)]


def bell_draw(rng, extent, scale, reach, cuts=(), held_as=jnp.bfloat16):
    result = scale * jax.random.normal(rng, extent, jnp.float32)
    if cuts:
        result = result * block_scale(rng, extent, cuts, -0.22, 0.18)
    return jnp.clip(result, -reach, reach).astype(held_as)


def setup_inputs(seed: int = 0) -> dict:
    streams_of = jax.random.split(jax.random.key(seed), 11)
    return {
        "hidden_in": bell_draw(streams_of[0], (TOKENS, D), 0.25, 1.5, ((0, 64),)),
        "w_query": draw_w_query(jax.random.fold_in(streams_of[10], 71), 0),
        "w_key": draw_w_key(jax.random.fold_in(streams_of[10], 71), 0),
        "w_value": draw_w_value(jax.random.fold_in(streams_of[10], 71), 0),
        "w_out": draw_w_out(jax.random.fold_in(streams_of[10], 71), 0),
        "value_weight": bell_draw(streams_of[5], (D,), D ** -0.5, 0.09375, ((0, 8),), jnp.float32),
        "rewards": bell_draw(streams_of[6], (TOKENS,), 0.1, 0.6, ((0, 64),), jnp.float32),
        "old_values": bell_draw(streams_of[7], (TOKENS,), 1.0, 6.0, ((0, 64),), jnp.float32),
        "lengths": ragged_sizes(streams_of[8], EPISODES, TOKENS, MAX_LEN, 2).astype(jnp.int32),
        "terminal": touch_ends((jax.random.randint(streams_of[9], (EPISODES,), 0, 2) < 1).astype(jnp.int32), jax.random.fold_in(streams_of[9], 1), 0, 1),
    }


discount = 0.999
trace_decay = 0.997
clip_range = 0.2
epsilon = 1e-05
rope_base = 500000.0

def rotate(states, positions):
    half = HEAD // 2
    freq = rope_base ** (-jnp.arange(half, dtype=jnp.float32) * 2.0 / HEAD)
    angles = positions[:, None] * freq[None, :]
    cosine = jnp.cos(angles)[:, None, :]
    sine = jnp.sin(angles)[:, None, :]
    first = states[..., :half]
    second = states[..., half:]
    return jnp.concatenate([first * cosine - second * sine, second * cosine + first * sine], -1)

def episode_marks(lengths, terminal, position_ids):
    ends = jnp.cumsum(lengths).astype(jnp.int32)
    matches = ends[None, :] - 1 == position_ids[:, None]
    finished = jnp.any(matches, 1).astype(jnp.float32)
    stopped = lax.optimization_barrier(jnp.sum(jnp.where(matches, terminal[None, :], 0), 1)).astype(jnp.float32)
    episode = lax.optimization_barrier(jnp.sum((ends[None, :] <= position_ids[:, None]).astype(jnp.int32), 1))
    return (finished, stopped, episode)

def attend_window(inputs):
    query, key, values_proj, episode = inputs
    rows = query.shape[0]
    group = HEADS // KV_HEADS
    q_four = query.astype(jnp.float32).reshape(rows, KV_HEADS, group, HEAD)
    k_four = key.astype(jnp.float32).reshape(rows, KV_HEADS, HEAD)
    v_four = values_proj.astype(jnp.float32).reshape(rows, KV_HEADS, HEAD)
    scores = jnp.einsum('tkgd,skd->kgts', q_four, k_four) * (1.0 / HEAD ** 0.5)
    order = jnp.arange(rows, dtype=jnp.int32)
    allowed = (order[None, :] <= order[:, None]) & (episode[None, :] == episode[:, None])
    masked = jnp.where(allowed[None, None], scores, -1e+30)
    largest = lax.optimization_barrier(jnp.max(masked, -1, keepdims=True))
    expon = jnp.where(allowed[None, None], jnp.exp(masked - largest), 0.0)
    probs = (expon / lax.optimization_barrier(jnp.sum(expon, -1, keepdims=True))).astype(jnp.bfloat16)
    output = jnp.einsum('kgts,skd->tkgd', probs.astype(jnp.float32), v_four)
    return output.astype(jnp.bfloat16).reshape(rows, HEADS * HEAD)

def reference(hidden_in, w_query, w_key, w_value, w_out, value_weight, rewards, old_values, lengths, terminal):
    states = hidden_in.astype(jnp.float32)
    normed = (states * lax.rsqrt(lax.optimization_barrier(jnp.mean(states * states, 1, keepdims=True)) + epsilon)).astype(jnp.bfloat16)
    position_ids = jnp.arange(TOKENS, dtype=jnp.int32)
    positions = position_ids.astype(jnp.float32)
    query = jnp.dot(normed, w_query, preferred_element_type=jnp.float32).reshape(TOKENS, HEADS, HEAD)
    query = rotate(query, positions).astype(jnp.bfloat16)
    key = jnp.dot(normed, w_key, preferred_element_type=jnp.float32).reshape(TOKENS, KV_HEADS, HEAD)
    key = rotate(key, positions).astype(jnp.bfloat16)
    values_proj = jnp.dot(normed, w_value, preferred_element_type=jnp.float32).astype(jnp.bfloat16)
    finished, stopped, episode = episode_marks(lengths, terminal, position_ids)
    windows = (query.reshape(N_DP, TOK_DEV, HEADS * HEAD), key.reshape(N_DP, TOK_DEV, KV_HEADS * HEAD), values_proj.reshape(N_DP, TOK_DEV, KV_HEADS * HEAD), episode.reshape(N_DP, TOK_DEV))
    attended = lax.map(attend_window, windows).reshape(TOKENS, HEADS * HEAD)
    residual = states + jnp.dot(attended, w_out, preferred_element_type=jnp.float32)
    value = lax.optimization_barrier(jnp.sum(residual * value_weight[None, :], 1)) * lax.rsqrt(lax.optimization_barrier(jnp.mean(residual * residual, 1)) + epsilon)
    next_old = jnp.concatenate([old_values[1:], jnp.zeros((1,), jnp.float32)])
    booted = jnp.where(finished > 0, (1.0 - stopped) * old_values, next_old)
    delta = rewards + discount * booted - old_values
    carried = discount * trace_decay * (1.0 - finished)

    def backward(carry, item):
        step_delta, step_keep = item
        fresh = step_delta + step_keep * carry
        return (fresh, fresh)
    _, advantage = lax.scan(backward, jnp.zeros((), jnp.float32), (delta, carried), reverse=True)
    returns = advantage + old_values
    clipped = old_values + jnp.clip(value - old_values, -clip_range, clip_range)
    terms = jnp.maximum((value - returns) ** 2, (clipped - returns) ** 2)
    value_loss = 0.5 * jnp.sum(terms) / TOKENS
    return (value, advantage, value_loss)
```

```python
import functools
import math

import jax
import jax.numpy as jnp
from jax import lax
from jax.experimental import pallas as pl
from jax.experimental.pallas import tpu as pltpu
from jax.sharding import PartitionSpec as P

HEAD = 128
discount = 0.999
trace_decay = 0.997
clip_range = 0.2
epsilon = 1e-05
rope_base = 500000.0

MESH = pl.DeviceIdType.MESH
F32 = jnp.float32
BF16 = jnp.bfloat16


def kernel(
    nz, nx,
    hid_hbm, wq_hbm, wk_hbm, wv_hbm, wo_hbm, cs_ref, sn_ref, vw_ref, rew_ref, old_ref, len_ref, term_ref,
    val_ref, adv_ref, loss_ref,
    hid, hown, wq, wkv, wo, att, accq, acckv, qs, ks, vs, bias, acco, rows_s, gae, red, lz, ly,
    lsem, rq, rkv, ro, ratt, rred, rlz, rly, rgae, ssem,
):
    D = hid.shape[1]
    T = hid.shape[0]
    R = wq_hbm.shape[0]
    FQ = wq_hbm.shape[1]
    FK = wk_hbm.shape[1]
    heads = FQ // HEAD
    nwin = gae.shape[0]
    ndp = 4 * nz
    half = nz // 2

    d = lax.axis_index("dp")
    m = lax.axis_index("mp")
    c = lax.rem(d, 2)
    z = lax.rem(d // 2, nz)
    yl = d // (2 * nz)
    yo = 1 - yl
    co = 1 - c
    xh = lax.rem(m, nx)
    yh = m // nx

    def dpi(yy, zz, cc):
        return (yy * nz + zz) * 2 + cc

    def zat(k):
        return lax.rem(z + (2 * nz + k), nz)

    def mpi(hh, k):
        return hh * nx + lax.rem(xh + (2 * nx + k), nx)

    def dev(dd, mm):
        return {"dp": dd, "mp": mm}

    sib = dev(dpi(yl, z, co), m)
    ypart = dev(dpi(yo, z, c), m)

    def zdev(k):
        return dev(dpi(yl, zat(k), c), m)

    def wslot(buf, idx, count=1):
        return buf.at[pl.ds(pl.multiple_of(idx * R, R), count * R)]

    class Stream:
        def __init__(self, buf, sems, send):
            self.buf, self.sems, self.sendsem = buf, sems, send

        def send(self, idx, to):
            ref = wslot(self.buf, idx)
            pltpu.make_async_remote_copy(ref, ref, ssem.at[self.sendsem], self.sems.at[idx], device_id=to, device_id_type=MESH).start()

        def wait(self, idx):
            ref = wslot(self.buf, idx)
            pltpu.make_async_remote_copy(ref, ref, ssem.at[self.sendsem], self.sems.at[idx], device_id=sib, device_id_type=MESH).wait_recv()

        def drain(self, count):
            ref = wslot(self.buf, 0, count)
            pltpu.make_async_remote_copy(ref, ref, ssem.at[self.sendsem], self.sems.at[0], device_id=sib, device_id_type=MESH).wait_send()

    SQ = Stream(wq, rq, 0)
    SKV = Stream(wkv, rkv, 1)
    SO = Stream(wo, ro, 2)

    own = pl.ds(pl.multiple_of(d * R, R), R)
    copies = [
        pltpu.make_async_copy(wk_hbm, wkv.at[own, pl.ds(0, FK)], lsem.at[0]),
        pltpu.make_async_copy(wv_hbm, wkv.at[own, pl.ds(FK, FK)], lsem.at[1]),
        pltpu.make_async_copy(wq_hbm, wq.at[own], lsem.at[2]),
        pltpu.make_async_copy(wo_hbm, wo.at[own], lsem.at[3]),
        pltpu.make_async_copy(hid_hbm, hid, lsem.at[4]),
        pltpu.make_async_copy(
            hid_hbm.at[:, pl.ds(pl.multiple_of(m * FQ, FQ), FQ)], hown, lsem.at[5]
        ),
    ]
    for copy in copies:
        copy.start()

    peers = [zdev(1), zdev(-1), sib, ypart]
    mpeers = [lax.rem(m + k, 2 * nx) for k in range(1, 2 * nx)]
    peers += [dev(d, mm) for mm in mpeers]
    for k in range(1, nwin):
        peers += [dev(lax.rem(d + k, ndp), m), dev(lax.rem(d + ndp - k, ndp), m)]
    barrier = pltpu.get_barrier_semaphore()
    for peer in peers:
        pl.semaphore_signal(barrier, inc=1, device_id=peer, device_id_type=MESH)

    gae[0, pl.ds(0, 1), :] = rew_ref[...]
    gae[0, pl.ds(1, 1), :] = old_ref[...]
    for copy in copies[:3]:
        copy.wait()
    pl.semaphore_wait(barrier, len(peers))

    SKV.send(d, ypart)
    for k in (1, -1):
        SQ.send(d, zdev(k))
        SKV.send(d, zdev(k))
    SQ.send(d, ypart)
    SKV.send(d, sib)
    SQ.send(d, sib)
    for k in range(1, nwin):
        pltpu.make_async_remote_copy(
            gae.at[0], gae.at[k], ssem.at[4], rgae.at[k],
            device_id=dev(lax.rem(d + ndp - k, ndp), m), device_id_type=MESH,
        ).start()
    other = dpi(yo, z, c)
    SKV.wait(other)
    for k in (1, -1):
        SKV.send(other, zdev(k))
    SKV.send(other, sib)

    def qkv_step(s, q_in=(True, True), kv_in=(True, True), q_out=(True, True), kv_out=(True, True)):
        for n, sgn in enumerate((1, -1)):
            zo = zat(-sgn * s)
            if q_in[n]:
                iq = dpi(yl, zo, c)
                SQ.wait(iq)
                if q_out[n]:
                    SQ.send(iq, zdev(sgn))
                SQ.send(iq, ypart)
                SQ.send(iq, sib)
            if kv_in[n]:
                for yy in (yl, yo):
                    ik = dpi(yy, zo, c)
                    SKV.wait(ik)
                    if kv_out[n]:
                        SKV.send(ik, zdev(sgn))
                    SKV.send(ik, sib)

    def across(zz):
        iq = dpi(yo, zz, c)
        SQ.wait(iq)
        SQ.send(iq, sib)

    def across_step(s):
        across(zat(-s))
        across(zat(s))

    def wo_first():
        SO.wait(other)
        for k in (1, -1):
            SO.send(d, zdev(k))
            SO.send(other, zdev(k))
        SO.send(d, sib)
        SO.send(other, sib)

    def wo_step(s):
        last = s == half
        for n, sgn in enumerate((1, -1)):
            zo = zat(-sgn * s)
            for r, yy in enumerate((yl, yo)):
                if last and r != n:
                    continue
                io = dpi(yy, zo, c)
                SO.wait(io)
                if not last and (s != half - 1 or r == n):
                    SO.send(io, zdev(sgn))
                SO.send(io, sib)

    def norm_rows(i, _):
        rr = pl.ds(pl.multiple_of(i * 32, 32), 32)
        x = hid[rr, :].astype(F32)
        ms = jnp.sum(x * x, axis=1, keepdims=True) * (1.0 / D)
        hid[rr, :] = (x * lax.rsqrt(ms + epsilon)).astype(BF16)
        return 0

    def mm_pos(zz):
        for yy in (yl, yo):
            i = dpi(yy, zz, co)
            SQ.wait(i)
            SKV.wait(i)
        lhs, rq_, rkv_ = [], [], []
        for yy in (0, 1):
            r0 = pl.ds(pl.multiple_of(dpi(yy, zz, 0) * R, 2 * R), 2 * R)
            lhs.append(hid[:, r0])
            rq_.append(wq[r0, :])
            rkv_.append(wkv[r0, :])
        lhs = jnp.concatenate(lhs, axis=1)
        accq[...] += jnp.dot(lhs, jnp.concatenate(rq_, axis=0), preferred_element_type=F32)
        acckv[...] += jnp.dot(lhs, jnp.concatenate(rkv_, axis=0), preferred_element_type=F32)

    def mm_range(lo, hi):
        def step(i, _):
            dist = (i + 1) // 2
            k = dist * (1 - 2 * lax.rem(i, 2))
            mm_pos(lax.rem(z + nz + k, nz))
            return 0
        lax.fori_loop(lo, hi, step, 0)

    kappa = math.log(discount * trace_decay)

    def marks():
        nl = len_ref.shape[1]
        si = lax.broadcasted_iota(jnp.int32, (nl, nl), 0)
        li = lax.broadcasted_iota(jnp.int32, (nl, nl), 1)
        lens = len_ref[...].astype(F32)
        ends_col = jnp.sum(jnp.where(li <= si, lens, 0.0), axis=1, keepdims=True)
        ends_row = jnp.sum(jnp.where(li == si, ends_col, 0.0), axis=0, keepdims=True)
        term_col = jnp.sum(jnp.where(li == si, term_ref[...].astype(F32), 0.0), axis=1, keepdims=True)
        for k in range(1, nwin):
            pltpu.make_async_remote_copy(
                gae.at[0], gae.at[k], ssem.at[4], rgae.at[k], device_id=sib, device_id_type=MESH
            ).wait_recv()
        lane = lax.broadcasted_iota(jnp.int32, (1, T), 1)
        base = (d * T).astype(F32)
        for k in range(nwin):
            pos = base + (lane + k * T).astype(F32)
            ep = jnp.sum(jnp.where(ends_col <= pos, 1.0, 0.0), axis=0, keepdims=True)
            hit = (ends_col - 1.0) == pos
            fin = jnp.sum(jnp.where(hit, 1.0, 0.0), axis=0, keepdims=True)
            stp = jnp.sum(jnp.where(hit, term_col, 0.0), axis=0, keepdims=True)
            rew = gae[k, pl.ds(0, 1), :]
            old = gae[k, pl.ds(1, 1), :]
            nxt = pltpu.roll(old, T - 1, 1)
            if k + 1 < nwin:
                nxt = jnp.where(lane == T - 1, gae[k + 1, pl.ds(1, 1), :][:, :1], nxt)
            booted = jnp.where(fin > 0.0, (1.0 - stp) * old, nxt)
            delta = rew + discount * booted - old
            rows_s[pl.ds(k, 1), :] = ep
            rows_s[pl.ds(8 + k, 1), :] = delta * jnp.exp((lane + k * T).astype(F32) * kappa)

        def rowblock(r, advr):
            n = 64
            sub = r * n + lax.broadcasted_iota(jnp.int32, (n, 1), 0)
            posc = base + sub.astype(F32)
            epc = jnp.sum(jnp.where(ends_row <= posc, 1.0, 0.0), axis=1, keepdims=True)
            ll = lax.broadcasted_iota(jnp.int32, (n, T), 1)
            ss = r * n + lax.broadcasted_iota(jnp.int32, (n, T), 0)
            same = rows_s[pl.ds(0, 1), :] == epc
            bias[pl.ds(pl.multiple_of(r * n, n), n), :] = jnp.where((ll <= ss) & same, 0.0, -1e30)
            tot = jnp.where((ll >= ss) & same, rows_s[pl.ds(8, 1), :], 0.0)
            for k in range(1, nwin):
                tot += jnp.where(rows_s[pl.ds(k, 1), :] == epc, rows_s[pl.ds(8 + k, 1), :], 0.0)
            col = jnp.sum(tot, axis=1, keepdims=True) * jnp.exp(sub.astype(F32) * (-kappa))
            return advr + jnp.sum(jnp.where(ll == ss, col, 0.0), axis=0, keepdims=True)

        adv_ref[...] = lax.fori_loop(0, T // 64, rowblock, jnp.zeros((1, T), F32))

    accq[...] = jnp.zeros_like(accq)
    acckv[...] = jnp.zeros_like(acckv)
    copies[4].wait()
    lax.fori_loop(0, T // 64, norm_rows, 0)
    qkv_step(1)
    across(z)
    lax.fori_loop(T // 64, T // 32, norm_rows, 0)
    qkv_step(2)
    across_step(1)
    marks()

    def mid(s, _):
        qkv_step(s)
        across_step(s - 1)
        mm_range(2 * s - 6, 2 * s - 4)
        return 0

    lax.fori_loop(3, half - 1, mid, 0)
    copies[3].wait()
    SO.send(d, ypart)
    qkv_step(half - 1, q_out=(True, False), kv_out=(False, True))
    across_step(half - 2)
    wo_first()
    qkv_step(half, q_in=(True, False), kv_in=(False, True), q_out=(False, False), kv_out=(False, False))
    across_step(half - 1)
    across(zat(half))
    mm_range(2 * half - 8, nz)

    def rope(x):
        return (x * cs_ref[...] + pltpu.roll(x, HEAD // 2, 1) * sn_ref[...]).astype(BF16)

    for h in range(heads):
        qs[h] = rope(accq[:, h * HEAD:(h + 1) * HEAD])
    ks[...] = rope(acckv[:, :FK])
    vs[...] = acckv[:, FK:].astype(BF16)

    scale = 1.0 / HEAD**0.5
    xp, xm = dev(d, mpi(yh, 1)), dev(d, mpi(yh, -1))
    yx = dev(d, mpi(1 - yh, 0))

    def att_send(o, h, to):
        i = o * heads + h
        pltpu.make_async_remote_copy(
            att.at[i], att.at[i], ssem.at[3], ratt.at[i], device_id=to, device_id_type=MESH
        ).start()

    def att_wait(o, h):
        i = o * heads + h
        pltpu.make_async_remote_copy(
            att.at[i], att.at[i], ssem.at[3], ratt.at[i], device_id=sib, device_id_type=MESH
        ).wait_recv()

    QB = 128

    def head(h):
        for i in range(T // QB):
            n = (i + 1) * QB
            sc = lax.dot_general(
                qs[h, i * QB:n, :], ks[:n, :], (((1,), (1,)), ((), ())), preferred_element_type=F32
            ) * scale + bias[i * QB:n, :n]
            big = jnp.max(sc, axis=1, keepdims=True)
            ex = jnp.exp(sc - big)
            pr = (ex / jnp.sum(ex, axis=1, keepdims=True)).astype(BF16)
            out = jnp.dot(pr, vs[:n, :], preferred_element_type=F32)
            att[m * heads + h, i * QB:n, :] = out.astype(BF16)

    def head_send(h):
        att_send(m, h, xp)
        att_send(m, h, xm)
        att_send(m, h, yx)

    def head_step(h, _):
        head(h)
        head_send(h)
        return 0

    lax.fori_loop(0, 2, head_step, 0)
    wo_step(1)
    lax.fori_loop(2, heads, head_step, 0)
    wo_step(2)

    def relay_near(h):
        for k in (-1, 1):
            o = mpi(yh, k)
            att_wait(o, h)
            if (h % 2 == 0) == (k == -1):
                att_send(o, h, xp if k == -1 else xm)

    def relay_y(h):
        o = mpi(1 - yh, 0)
        att_wait(o, h)
        att_send(o, h, xp)
        att_send(o, h, xm)

    def relay_far(h):
        for k in (-1, 1):
            o = mpi(1 - yh, k)
            att_wait(o, h)
            if (h % 2 == 0) == (k == -1):
                att_send(o, h, xp if k == -1 else xm)

    relay_near(0)
    relay_y(0)
    wo_step(3)
    relay_near(1)
    relay_y(1)
    wo_step(4)
    relay_near(2)
    relay_y(2)
    wo_step(5)
    relay_near(3)
    relay_y(3)
    wo_step(6)
    relay_far(0)
    wo_step(7)
    relay_far(1)
    wo_step(8)

    def wo_rest(i, _):
        for yy in (0, 1):
            SO.wait(dpi(yy, i, co))
        return 0

    lax.fori_loop(0, nz, wo_rest, 0)

    def project(o):
        lhs = jnp.concatenate([att[o * heads + h] for h in range(heads)], axis=1)
        r0 = pl.ds(pl.multiple_of(o * FQ, FQ), FQ)
        acco[...] += jnp.dot(lhs, wo[r0, :], preferred_element_type=F32)

    copies[5].wait()
    acco[...] = hown[...].astype(F32)
    project(m)
    relay_far(2)
    project(mpi(yh, 1))
    project(mpi(yh, -1))
    project(mpi(1 - yh, 0))
    relay_far(3)
    project(mpi(1 - yh, 1))
    project(mpi(1 - yh, -1))
    for h in range(heads):
        att_wait(mpi(yh, 2), h)
    project(mpi(yh, 2))
    for h in range(heads):
        att_wait(mpi(1 - yh, 2), h)
    project(mpi(1 - yh, 2))

    def sums(r, carry):
        n = 64
        x = acco[pl.ds(pl.multiple_of(r * n, n), n), :]
        ll = lax.broadcasted_iota(jnp.int32, (n, T), 1)
        ss = r * n + lax.broadcasted_iota(jnp.int32, (n, T), 0)
        sq = jnp.sum(x * x, axis=1, keepdims=True)
        hs = jnp.sum(x * vw_ref[...], axis=1, keepdims=True)
        a, b = carry
        a = a + jnp.sum(jnp.where(ll == ss, sq, 0.0), axis=0, keepdims=True)
        b = b + jnp.sum(jnp.where(ll == ss, hs, 0.0), axis=0, keepdims=True)
        return a, b

    zero = jnp.zeros((1, T), F32)
    sq, hs = lax.fori_loop(0, T // 64, sums, (zero, zero))
    red[m, pl.ds(0, 1), :] = sq
    red[m, pl.ds(1, 1), :] = hs
    for mm in mpeers:
        pltpu.make_async_remote_copy(
            red.at[m], red.at[m], ssem.at[5], rred.at[m], device_id=dev(d, mm), device_id_type=MESH
        ).start()
    for mm in mpeers:
        pltpu.make_async_remote_copy(
            red.at[mm], red.at[mm], ssem.at[5], rred.at[mm], device_id=sib, device_id_type=MESH
        ).wait_recv()
    tot = red[0]
    for k in range(1, 2 * nx):
        tot = tot + red[k]
    value = tot[1:2] * lax.rsqrt(tot[0:1] * (1.0 / D) + epsilon)
    val_ref[...] = value
    old = old_ref[...]
    returns = adv_ref[...] + old
    clipped = old + jnp.clip(value - old, -clip_range, clip_range)
    terms = jnp.maximum((value - returns) ** 2, (clipped - returns) ** 2)
    part = jnp.sum(terms, axis=1, keepdims=True)

    lz[z] = jnp.broadcast_to(part, lz.shape[1:])
    for k in range(1, nz):
        pltpu.make_async_remote_copy(
            lz.at[z], lz.at[z], ssem.at[6], rlz.at[z], device_id=zdev(k), device_id_type=MESH
        ).start()
    for k in range(1, nz):
        zz = zat(k)
        pltpu.make_async_remote_copy(
            lz.at[zz], lz.at[zz], ssem.at[6], rlz.at[zz], device_id=sib, device_id_type=MESH
        ).wait_recv()
    part = lz[0]
    for k in range(1, nz):
        part = part + lz[k]
    me = yl * 2 + c
    ly[me] = part
    quad = [(yl, co), (yo, c), (yo, co)]
    for yy, cc in quad:
        pltpu.make_async_remote_copy(
            ly.at[me], ly.at[me], ssem.at[7], rly.at[me], device_id=dev(dpi(yy, z, cc), m), device_id_type=MESH
        ).start()
    for yy, cc in quad:
        i = yy * 2 + cc
        pltpu.make_async_remote_copy(
            ly.at[i], ly.at[i], ssem.at[7], rly.at[i], device_id=sib, device_id_type=MESH
        ).wait_recv()
    total = (ly[0] + ly[1]) + (ly[2] + ly[3])
    loss_ref[...] = total[0:1] * (0.5 / (T * ndp))

    SQ.drain(ndp - 1)
    SKV.drain(ndp - 1)
    SO.drain(ndp - 1)

    def drain(buf, sem, count):
        ref = buf.at[pl.ds(0, count)]
        pltpu.make_async_remote_copy(
            ref, ref, ssem.at[sem], rred.at[0], device_id=sib, device_id_type=MESH
        ).wait_send()

    drain(att, 3, 28)
    drain(gae, 4, nwin - 1)
    drain(red, 5, 2 * nx - 1)
    drain(lz, 6, nz - 1)
    drain(ly, 7, 3)


def solution(mesh):
    ndp, nmp = mesh.shape["dp"], mesh.shape["mp"]
    nz, nx = ndp // 4, nmp // 2
    nwin = 5

    def body(hidden_in, w_query, w_key, w_value, w_out, value_weight, rewards, old_values, lengths, terminal):
        T, D = hidden_in.shape
        R, FQ = w_query.shape
        FK = w_key.shape[1]
        heads = FQ // HEAD
        nl = lengths.shape[0]
        half = HEAD // 2
        positions = (lax.axis_index("dp") * T + jnp.arange(T, dtype=jnp.int32)).astype(F32)
        freq = rope_base ** (-jnp.arange(half, dtype=F32) * 2.0 / HEAD)
        angles = positions[:, None] * jnp.concatenate([freq, freq])[None, :]
        sign = jnp.concatenate([-jnp.ones((half,), F32), jnp.ones((half,), F32)])
        cosine, sine = jnp.cos(angles), jnp.sin(angles) * sign[None, :]
        any_ = pl.BlockSpec(memory_space=pl.ANY)
        vmem = pl.BlockSpec(memory_space=pltpu.VMEM)
        dma = pltpu.SemaphoreType.DMA
        value, advantage, loss = pl.pallas_call(
            functools.partial(kernel, nz, nx),
            out_shape=(
                jax.ShapeDtypeStruct((1, T), F32),
                jax.ShapeDtypeStruct((1, T), F32),
                jax.ShapeDtypeStruct((1, 128), F32),
            ),
            in_specs=[any_] * 5 + [vmem] * 7,
            out_specs=(vmem, vmem, vmem),
            scratch_shapes=[
                pltpu.VMEM((T, D), BF16),
                pltpu.VMEM((T, FQ), BF16),
                pltpu.VMEM((D, FQ), BF16),
                pltpu.VMEM((D, 2 * FK), BF16),
                pltpu.VMEM((D, FQ), BF16),
                pltpu.VMEM((nmp * heads, T, HEAD), BF16),
                pltpu.VMEM((T, FQ), F32),
                pltpu.VMEM((T, 2 * FK), F32),
                pltpu.VMEM((heads, T, HEAD), BF16),
                pltpu.VMEM((T, HEAD), BF16),
                pltpu.VMEM((T, HEAD), BF16),
                pltpu.VMEM((T, T), F32),
                pltpu.VMEM((T, FQ), F32),
                pltpu.VMEM((16, T), F32),
                pltpu.VMEM((nwin, 8, T), F32),
                pltpu.VMEM((nmp, 8, T), F32),
                pltpu.VMEM((nz, 8, 128), F32),
                pltpu.VMEM((4, 8, 128), F32),
                dma((6,)),
                dma((ndp,)),
                dma((ndp,)),
                dma((ndp,)),
                dma((nmp * heads,)),
                dma((nmp,)),
                dma((nz,)),
                dma((4,)),
                dma((nwin,)),
                dma((8,)),
            ],
            compiler_params=pltpu.CompilerParams(collective_id=0, has_side_effects=True),
        )(
            hidden_in, w_query, w_key, w_value, w_out, cosine, sine,
            value_weight.reshape(1, FQ), rewards.reshape(1, T), old_values.reshape(1, T),
            lengths.reshape(1, nl), terminal.reshape(1, nl),
        )
        return value.reshape(T), advantage.reshape(T), loss[0, 0]

    return jax.shard_map(
        body,
        mesh=mesh,
        in_specs=(
            P("dp", None), P("dp", "mp"), P("dp", "mp"), P("dp", "mp"), P("dp", "mp"),
            P("mp"), P("dp"), P("dp"), P(), P(),
        ),
        out_specs=(P("dp"), P("dp"), P()),
        check_vma=False,
    )
```

```python
import functools
import math

import jax
import jax.numpy as jnp
from jax import lax
from jax.experimental import pallas as pl
from jax.experimental.pallas import tpu as pltpu
from jax.sharding import PartitionSpec as P

HEAD = 128
discount = 0.999
trace_decay = 0.997
clip_range = 0.2
epsilon = 1e-05
rope_base = 500000.0

MESH = pl.DeviceIdType.MESH
F32 = jnp.float32
BF16 = jnp.bfloat16


CUT = 3


def att_numbers(heads):
    bulk, own = [0] * 5, {}
    kinds = ["near", "two", "y", "far", "last"]
    table = {}
    for kind, k, p in [(kind, k, p) for kind in kinds for k in ((-1, 1) if kind in ("near", "far") else (0,)) for p in range(2 * heads)]:
        turn = (p % 2 == 0) == (k == -1)
        passed = {
            "near": turn or p < CUT, "two": p < CUT, "y": p >= CUT, "far": turn and p >= CUT, "last": False
        }[kind]
        if passed:
            table[kind, k, p] = 5 + len(own)
            own[kind, k, p] = True
        else:
            table[kind, k, p] = kinds.index(kind)
            bulk[kinds.index(kind)] += 1
    return (lambda kind, k, p: table[kind, k, p]), bulk


def att_sems(heads):
    number, bulk = att_numbers(heads)
    return 1 + max(number(kind, k, p) for kind, k in (("near", -1), ("near", 1), ("two", 0), ("y", 0), ("far", -1), ("far", 1), ("last", 0)) for p in range(2 * heads))


def kernel(
    nz, nx,
    hid_hbm, wq_hbm, wk_hbm, wv_hbm, wo_hbm, cs_hbm, sn_hbm, vw_hbm, rew_hbm, old_hbm, len_hbm, term_hbm,
    out_hbm, loss_hbm,
    cs_ref, sn_ref, vw_ref, rew_ref, old_ref, len_ref, term_ref, val_ref, adv_ref, loss_ref,
    hid, hown, wq, wkv, wo, att, accq, acckv, qs, ks, vs, bias, acco, rows_s, gae, red, lz,
    lsem, rq, rkv, ro, ratt, rmisc, ssem,
):
    D = hid.shape[1]
    T = hid.shape[0]
    R = wq_hbm.shape[0]
    FQ = wq_hbm.shape[1]
    FK = wk_hbm.shape[1]
    heads = FQ // HEAD
    nwin = gae.shape[0]
    ndp = 4 * nz
    half = nz // 2

    d = lax.axis_index("dp")
    m = lax.axis_index("mp")
    c = lax.rem(d, 2)
    z = lax.rem(d // 2, nz)
    yl = d // (2 * nz)
    yo = 1 - yl
    co = 1 - c
    xh = lax.rem(m, nx)
    yh = m // nx

    def dpi(yy, zz, cc):
        return (yy * nz + zz) * 2 + cc

    def zat(k):
        return lax.rem(z + (2 * nz + k), nz)

    def mpi(hh, k):
        return hh * nx + lax.rem(xh + (2 * nx + k), nx)

    def dev(dd, mm):
        return {"dp": dd, "mp": mm}

    sib = dev(dpi(yl, z, co), m)
    ypart = dev(dpi(yo, z, c), m)

    def zdev(k):
        return dev(dpi(yl, zat(k), c), m)

    def wslot(buf, idx, n, count=1):
        return buf.at[pl.ds(pl.multiple_of(idx * n, n), count * n)]

    class Stream:
        def __init__(self, buf, send, n):
            self.buf, self.sendsem, self.n = buf, send, n

        def copy(self, ref, sem, to):
            return pltpu.make_async_remote_copy(ref, ref, ssem.at[self.sendsem], sem, device_id=to, device_id_type=MESH)

        def send(self, idx, sem, to):
            self.copy(wslot(self.buf, idx, self.n), sem, to).start()

        def wait(self, sem, count=1):
            self.copy(wslot(self.buf, 0, self.n, count), sem, sib).wait_recv()

        def drain(self, count):
            self.copy(wslot(self.buf, 0, self.n, count), ssem.at[self.sendsem], sib).wait_send()

    SQ = Stream(wq, 0, R // 2)
    SKV = Stream(wkv, 1, R)
    SO = Stream(wo, 2, R)

    own = pl.ds(pl.multiple_of(d * R, R), R)
    copies = [
        pltpu.make_async_copy(wk_hbm, wkv.at[own, pl.ds(0, FK)], lsem.at[0]),
        pltpu.make_async_copy(wv_hbm, wkv.at[own, pl.ds(FK, FK)], lsem.at[1]),
        pltpu.make_async_copy(wq_hbm, wq.at[own], lsem.at[2]),
        pltpu.make_async_copy(wo_hbm, wo.at[own], lsem.at[3]),
        pltpu.make_async_copy(hid_hbm, hid, lsem.at[4]),
        pltpu.make_async_copy(
            hid_hbm.at[:, pl.ds(pl.multiple_of(m * FQ, FQ), FQ)], hown, lsem.at[5]
        ),
    ]
    small = [
        pltpu.make_async_copy(src, dst, lsem.at[6 + i])
        for i, (src, dst) in enumerate([
            (rew_hbm, rew_ref), (old_hbm, old_ref), (len_hbm, len_ref), (term_hbm, term_ref),
            (vw_hbm, vw_ref), (cs_hbm, cs_ref), (sn_hbm, sn_ref),
        ])
    ]
    outs = [
        pltpu.make_async_copy(src, dst, lsem.at[13 + i])
        for i, (src, dst) in enumerate([(adv_ref, out_hbm.at[1]), (val_ref, out_hbm.at[0]), (loss_ref, loss_hbm)])
    ]
    for copy in copies[:3]:
        copy.start()

    kappa = math.log(discount * trace_decay)

    nl = len_ref.shape[1]

    def ends():
        si = lax.broadcasted_iota(jnp.int32, (nl, nl), 0)
        li = lax.broadcasted_iota(jnp.int32, (nl, nl), 1)
        lens = len_ref[...].astype(F32)
        ends_col = jnp.sum(jnp.where(li <= si, lens, 0.0), axis=1, keepdims=True)
        return si, li, ends_col

    base = (d * T).astype(F32)
    lane = lax.broadcasted_iota(jnp.int32, (1, T), 1)

    def landed(buf, send, sem, count):
        ref = buf.at[pl.ds(0, count)]
        pltpu.make_async_remote_copy(ref, ref, ssem.at[send], sem, device_id=sib, device_id_type=MESH).wait_recv()

    def first_marks():
        si, li, ends_col = ends()
        rows_s[pl.ds(6, 1), pl.ds(0, nl)] = jnp.sum(jnp.where(li == si, ends_col, 0.0), axis=0, keepdims=True)
        pos = base + lane.astype(F32)
        rows_s[pl.ds(0, 1), :] = jnp.sum(jnp.where(ends_col <= pos, 1.0, 0.0), axis=0, keepdims=True)

    xp, xm = dev(d, mpi(yh, 1)), dev(d, mpi(yh, -1))
    yx = dev(d, mpi(1 - yh, 0))
    peers = [zdev(1), zdev(-1), sib, ypart, xp, xm, yx]
    mpeers = [lax.rem(m + k, 2 * nx) for k in range(1, 2 * nx)]
    barrier = pltpu.get_barrier_semaphore()
    for peer in peers:
        pl.semaphore_signal(barrier, inc=1, device_id=peer, device_id_type=MESH)
    for copy in copies[4:] + small + copies[3:4]:
        copy.start()
    for copy in copies[:3]:
        copy.wait()
    pl.semaphore_wait(barrier, len(peers))

    sgn = 2 * c - 1
    onward = zdev(sgn)

    other, theirs, both = dpi(yo, z, c), dpi(yl, z, co), dpi(yo, z, co)

    def q_ring(s, n, i):
        return rq.at[(s - 1) * 4 + n * 2 + i]

    def q_cross(k, n, i):
        return rq.at[4 * half - 2 + k * 4 + n * 2 + i]

    def q_sib(k):
        return rq.at[8 * half + k]

    def kv_ring(s, n, r):
        return rkv.at[(s - 1) * 4 + n * 2 + r]

    def kv_sib(k):
        return rkv.at[4 * half - 2 + k]

    def o_ring(s, n, r):
        return ro.at[(s - 1) * 4 + n * 2 + r]

    KV_Y, KV_THEIRS, KV_BOTH = (rkv.at[5 * half - 1 + k] for k in range(3))
    O_Y, O_THEIRS, O_BOTH, O_SIB = (ro.at[4 * half - 2 + k] for k in range(4))
    Q_THEIRS = rq.at[9 * half + 1]

    def core_of(n):
        return c if n == 0 else co

    def zat_(k):
        return lax.rem(z + 2 * nz + k, nz)

    def nothing():
        pass

    def kv_pass(s, zo, n, r, on):
        ik = dpi(yl if r == 0 else yo, zo, core_of(n))
        SKV.wait(kv_ring(s, n, r))
        if on:
            SKV.send(ik, kv_ring(s + 1, n, r), onward)
        SKV.send(ik, kv_sib(s - 1), sib)

    def across(k, n, i):
        iq = dpi(yo, zat_(-sgn * k), core_of(n)) * 2 + i
        SQ.wait(q_cross(k, n, i))
        SQ.send(iq, q_sib(k), sib)

    def qkv_step(s, pieces, cores=(0, 1), out=(0, 1)):
        zo = zat_(-sgn * s)
        todo = list(pieces)
        first = isinstance(s, int) and s == 1
        crossing = [(n, i) for n in ((0,) if first else (0, 1)) for i in (0, 1)]

        def work():
            if todo:
                todo.pop(0)()

        def cross_next():
            if crossing:
                across(s - 1, *crossing.pop(0))

        for n in cores:
            for i in (0, 1):
                iq = dpi(yl, zo, core_of(n)) * 2 + i
                SQ.wait(q_ring(s, n, i))
                if n in out:
                    SQ.send(iq, q_ring(s + 1, n, i), onward)
                SQ.send(iq, q_cross(s, n, i), ypart)
                SQ.send(iq, q_sib(s), sib)
                work()
            kv_pass(s, zo, n, 0, n in out)
            cross_next()
            work()
        for n in cores:
            kv_pass(s, zo, n, 1, n in out)
            cross_next()
            work()
        while crossing:
            cross_next()
        while todo:
            work()

    def wo_first():
        SO.send(d, o_ring(1, 0, 0), onward)
        SO.wait(O_THEIRS)
        SO.send(theirs, o_ring(1, 1, 0), onward)
        SO.wait(O_Y)
        SO.send(other, o_ring(1, 0, 1), onward)
        SO.send(other, O_BOTH, sib)
        SO.wait(O_BOTH)
        SO.send(both, o_ring(1, 1, 1), onward)

    def wo_step(s):
        zo = zat_(-sgn * s)
        for n in (0,) if s == half else (0, 1):
            for r, yy in enumerate((yl, yo)):
                io = dpi(yy, zo, core_of(n))
                SO.wait(o_ring(s, n, r))
                if s < half - 1 or (s == half - 1 and n == 0):
                    SO.send(io, o_ring(s + 1, n, r), onward)
                SO.send(io, O_SIB, sib)

    def norm_rows(i, _):
        rr = pl.ds(pl.multiple_of(i * 32, 32), 32)
        x = hid[rr, :].astype(F32)
        ms = jnp.sum(x * x, axis=1, keepdims=True) * (1.0 / D)
        hid[rr, :] = (x * lax.rsqrt(ms + epsilon)).astype(BF16)
        return 0

    def rows_of(zz):
        return [pl.ds(pl.multiple_of(dpi(yy, zz, 0) * R, 2 * R), 2 * R) for yy in (0, 1)]

    def mm_q(zz):
        lhs = jnp.concatenate([hid[:, r] for r in rows_of(zz)], axis=1)
        rhs = jnp.concatenate([wq[r, :] for r in rows_of(zz)], axis=0)
        accq[...] += jnp.dot(lhs, rhs, preferred_element_type=F32)

    def mm_kv(zz):
        lhs = jnp.concatenate([hid[:, r] for r in rows_of(zz)], axis=1)
        rhs = jnp.concatenate([wkv[r, :] for r in rows_of(zz)], axis=0)
        acckv[...] += jnp.dot(lhs, rhs, preferred_element_type=F32)

    def opp_q(k):
        SQ.wait(q_sib(k), 8)
        mm_q(zat_(sgn * k))

    def opp_kv(k):
        SKV.wait(kv_sib(k - 1), 4)
        mm_kv(zat_(sgn * k))

    NB = 64

    def block_of(r):
        sub = r * NB + lax.broadcasted_iota(jnp.int32, (NB, 1), 0)
        posc = base + sub.astype(F32)
        epc = jnp.sum(jnp.where(rows_s[pl.ds(6, 1), pl.ds(0, nl)] <= posc, 1.0, 0.0), axis=1, keepdims=True)
        ll = lax.broadcasted_iota(jnp.int32, (NB, T), 1)
        ss = r * NB + lax.broadcasted_iota(jnp.int32, (NB, T), 0)
        return sub, epc, ll, ss

    def bias_rows(r, _):
        sub, epc, ll, ss = block_of(r)
        same = rows_s[pl.ds(0, 1), :] == epc
        bias[pl.ds(pl.multiple_of(r * NB, NB), NB), :] = jnp.where((ll <= ss) & same, 0.0, -1e30)
        return 0

    def gae_send():
        for k in range(1, nwin):
            pltpu.make_async_remote_copy(
                gae.at[0], gae.at[k], ssem.at[4], rmisc.at[0],
                device_id=dev(lax.rem(d + ndp - k, ndp), m), device_id_type=MESH,
            ).start()

    def advantages():
        landed(gae, 4, rmisc.at[0], nwin - 1)
        si, li, ends_col = ends()
        term_col = jnp.sum(jnp.where(li == si, term_ref[...].astype(F32), 0.0), axis=1, keepdims=True)
        for k in range(nwin):
            pos = base + (lane + k * T).astype(F32)
            ep = jnp.sum(jnp.where(ends_col <= pos, 1.0, 0.0), axis=0, keepdims=True)
            hit = (ends_col - 1.0) == pos
            fin = jnp.sum(jnp.where(hit, 1.0, 0.0), axis=0, keepdims=True)
            stp = jnp.sum(jnp.where(hit, term_col, 0.0), axis=0, keepdims=True)
            rew = gae[k, pl.ds(0, 1), :]
            old = gae[k, pl.ds(1, 1), :]
            nxt = pltpu.roll(old, T - 1, 1)
            if k + 1 < nwin:
                nxt = jnp.where(lane == T - 1, gae[k + 1, pl.ds(1, 1), :][:, :1], nxt)
            booted = jnp.where(fin > 0.0, (1.0 - stp) * old, nxt)
            delta = rew + discount * booted - old
            rows_s[pl.ds(k, 1), :] = ep
            rows_s[pl.ds(8 + k, 1), :] = delta * jnp.exp((lane + k * T).astype(F32) * kappa)

        def rowblock(r, advr):
            sub, epc, ll, ss = block_of(r)
            same = rows_s[pl.ds(0, 1), :] == epc
            tot = jnp.where((ll >= ss) & same, rows_s[pl.ds(8, 1), :], 0.0)
            for k in range(1, nwin):
                tot += jnp.where(rows_s[pl.ds(k, 1), :] == epc, rows_s[pl.ds(8 + k, 1), :], 0.0)
            col = jnp.sum(tot, axis=1, keepdims=True) * jnp.exp(sub.astype(F32) * (-kappa))
            return advr + jnp.sum(jnp.where(ll == ss, col, 0.0), axis=0, keepdims=True)

        adv_ref[...] = lax.fori_loop(0, T // NB, rowblock, jnp.zeros((1, T), F32))
        outs[0].start()

    SKV.send(d, KV_Y, ypart)
    for i in (0, 1):
        SQ.send(2 * d + i, Q_THEIRS, sib)
    SKV.send(d, KV_THEIRS, sib)
    for i in (0, 1):
        SQ.send(2 * d + i, q_ring(1, 0, i), onward)
    SKV.send(d, kv_ring(1, 0, 0), onward)
    for i in (0, 1):
        SQ.send(2 * d + i, q_cross(0, 0, i), ypart)
    accq[...] = jnp.zeros_like(accq)
    acckv[...] = jnp.zeros_like(acckv)
    for copy in small + copies[4:5]:
        copy.wait()
    gae[0, pl.ds(0, 1), :] = rew_ref[...]
    gae[0, pl.ds(1, 1), :] = old_ref[...]
    first_marks()
    SQ.wait(Q_THEIRS, 2)
    for i in (0, 1):
        SQ.send(2 * theirs + i, q_ring(1, 1, i), onward)
    SKV.wait(KV_THEIRS)
    SKV.send(theirs, kv_ring(1, 1, 0), onward)
    lax.fori_loop(0, 4, norm_rows, 0)
    def norms(lo, hi):
        return functools.partial(lax.fori_loop, lo, hi, norm_rows, 0)

    def other_kv():
        SKV.wait(KV_Y)
        SKV.send(other, kv_ring(1, 0, 1), onward)
        SKV.send(other, KV_BOTH, sib)

    def both_kv():
        SKV.wait(KV_BOTH)
        SKV.send(both, kv_ring(1, 1, 1), onward)

    qkv_step(1, [norms(4, 5), other_kv, both_kv, norms(5, 6), norms(6, 7), norms(7, 8), norms(8, 9), norms(9, 10)])
    def biases(lo, hi):
        return functools.partial(lax.fori_loop, lo, hi, bias_rows, 0)

    def own_q():
        SQ.wait(q_sib(0), 2)
        mm_q(z)

    def own_kv():
        mm_kv(z)

    qkv_step(2, [norms(10, 11), norms(11, 12), norms(12, 13), norms(13, 14), norms(14, 15), norms(15, 16), own_kv, own_q])
    def pieces_at(s):
        k = s - 2
        zm = zat_(-sgn * k)
        return [nothing, lambda: mm_q(zm), nothing, lambda: mm_kv(zm), nothing, lambda: opp_q(k), nothing, lambda: opp_kv(k)]

    share = T // NB // (half - 4)

    def mid(s, _):
        extra = pieces_at(s)
        extra[0] = functools.partial(lax.fori_loop, (s - 3) * share, (s - 2) * share, bias_rows, 0)
        qkv_step(s, extra)
        return 0

    lax.fori_loop(3, half - 1, mid, 0)
    copies[3].wait()
    SO.send(d, O_THEIRS, sib)
    SO.send(d, O_Y, ypart)
    qkv_step(half - 1, pieces_at(half - 1), out=(0,))
    wo_first()
    qkv_step(half, pieces_at(half), cores=(0,), out=())
    mm_kv(zat_(-sgn * (half - 1)))
    mm_q(zat_(-sgn * (half - 1)))
    for i in (0, 1):
        across(half, 0, i)
    opp_kv(half - 1)
    opp_q(half - 1)
    SKV.wait(kv_sib(half - 1), 2)
    mm_kv(zat_(half))
    wo_step(1)
    SQ.wait(q_sib(half), 4)
    mm_q(zat_(half))

    low = lax.broadcasted_iota(jnp.int32, (T // 2, HEAD), 1) < HEAD // 2

    def spread(ref, sign):
        table = ref[...]
        turned = pltpu.roll(table, HEAD // 2, 1)
        first, second = jnp.where(low, table, turned), jnp.where(low, turned, table)
        if sign:
            first, second = jnp.where(low, -first, first), jnp.where(low, -second, second)
        return first, second

    cosines, sines = spread(cs_ref, False), spread(sn_ref, True)

    def rope(load, store):
        for n in (0, 1):
            x = load(slice(n * T // 2, (n + 1) * T // 2))
            store(slice(n * T // 2, (n + 1) * T // 2), (x * cosines[n] + pltpu.roll(x, HEAD // 2, 1) * sines[n]).astype(BF16))

    def put_q(h):
        def store(r, x):
            qs[h, r, :] = x
        return store

    def put_k(r, x):
        ks[r, :] = x

    for h in range(heads):
        rope(lambda r: accq[r, h * HEAD:(h + 1) * HEAD], put_q(h))
    rope(lambda r: acckv[r, :FK], put_k)
    vs[...] = acckv[:, FK:].astype(BF16)

    scale = 1.0 / HEAD**0.5

    number, bulk = att_numbers(heads)

    def att_copy(o, p, kind, k, to):
        i = o * (2 * heads) + p
        n = number(kind, k, p)
        return pltpu.make_async_remote_copy(
            att.at[i], att.at[i], ssem.at[3], ratt.at[n], device_id=to, device_id_type=MESH
        )

    def att_send(o, p, kind, k, to):
        att_copy(o, p, kind, k, to).start()

    def att_wait(o, p, kind, k):
        if number(kind, k, p) >= len(bulk):
            att_copy(o, p, kind, k, sib).wait_recv()

    def att_rest(n):
        landed(att, 3, ratt.at[n], bulk[n])

    QB = 128

    def piece_send(p):
        att_send(m, p, "near", -1, xp)
        att_send(m, p, "near", 1, xm)
        att_send(m, p, "y", 0, yx)

    def head_step(h):
        for i in range(T // QB):
            n = (i + 1) * QB
            sc = lax.dot_general(
                qs[h, i * QB:n, :], ks[:n, :], (((1,), (1,)), ((), ())), preferred_element_type=F32
            ) * scale + bias[i * QB:n, :n]
            big = jnp.max(sc, axis=1, keepdims=True)
            ex = jnp.exp(sc - big)
            pr = (ex / jnp.sum(ex, axis=1, keepdims=True)).astype(BF16)
            out = jnp.dot(pr, vs[:n, :], preferred_element_type=F32)
            r = 2 * i // (T // QB)
            low_row = i * QB - r * (T // 2)
            att[m * (2 * heads) + 2 * h + r, low_row:low_row + QB, :] = out.astype(BF16)
            if (i + 1) * 2 % (T // QB) == 0:
                piece_send(2 * h + r)

    head_step(0)
    head_step(1)
    gae_send()
    wo_step(2)
    for h in range(2, heads):
        head_step(h)

    cut = CUT

    def relay_near(p):
        for k in (-1, 1):
            o = mpi(yh, k)
            att_wait(o, p, "near", k)
            if (p % 2 == 0) == (k == -1):
                att_send(o, p, "two", 0, xp if k == -1 else xm)
            if p < cut:
                att_send(o, p, "far", k, yx)

    def relay_two(p):
        o = mpi(yh, 2)
        att_wait(o, p, "two", 0)
        if p < cut:
            att_send(o, p, "last", 0, yx)

    def relay_y(p):
        o = mpi(1 - yh, 0)
        att_wait(o, p, "y", 0)
        if p >= cut:
            att_send(o, p, "far", -1, xp)
            att_send(o, p, "far", 1, xm)

    def relay_far(p):
        for k in (-1, 1):
            o = mpi(1 - yh, k)
            att_wait(o, p, "far", k)
            if p >= cut and (p % 2 == 0) == (k == -1):
                att_send(o, p, "last", 0, xp if k == -1 else xm)

    for p in range(cut):
        relay_near(p)
    wo_step(3)
    advantages()
    wo_step(4)
    for p in range(cut, 2 * heads):
        relay_near(p)
        relay_y(p)
    wo_step(5)
    for p in range(cut):
        relay_two(p)
    wo_step(6)
    relay_far(3)
    relay_far(4)
    wo_step(7)
    relay_far(5)
    relay_far(6)
    wo_step(8)
    relay_far(7)

    SO.wait(O_SIB, 4 * half - 2)
    def project(o):
        r0 = pl.ds(pl.multiple_of(o * FQ, FQ), FQ)
        for r in (0, 1):
            lhs = jnp.concatenate([att[o * (2 * heads) + 2 * h + r] for h in range(heads)], axis=1)
            acco[r * T // 2:(r + 1) * T // 2, :] += jnp.dot(lhs, wo[r0, :], preferred_element_type=F32)

    copies[5].wait()
    acco[...] = hown[...].astype(F32)
    project(m)
    att_rest(0)
    project(mpi(yh, 1))
    project(mpi(yh, -1))
    att_rest(1)
    project(mpi(yh, 2))
    att_rest(2)
    project(mpi(1 - yh, 0))
    att_rest(3)
    project(mpi(1 - yh, 1))
    project(mpi(1 - yh, -1))
    att_rest(4)
    project(mpi(1 - yh, 2))

    def sums(r, carry):
        n = 64
        x = acco[pl.ds(pl.multiple_of(r * n, n), n), :]
        ll = lax.broadcasted_iota(jnp.int32, (n, T), 1)
        ss = r * n + lax.broadcasted_iota(jnp.int32, (n, T), 0)
        sq = jnp.sum(x * x, axis=1, keepdims=True)
        hs = jnp.sum(x * vw_ref[...], axis=1, keepdims=True)
        a, b = carry
        a = a + jnp.sum(jnp.where(ll == ss, sq, 0.0), axis=0, keepdims=True)
        b = b + jnp.sum(jnp.where(ll == ss, hs, 0.0), axis=0, keepdims=True)
        return a, b

    zero = jnp.zeros((1, T), F32)
    sq, hs = lax.fori_loop(0, T // 64, sums, (zero, zero))
    red[m, pl.ds(0, 1), :] = sq
    red[m, pl.ds(1, 1), :] = hs
    for mm in mpeers:
        pltpu.make_async_remote_copy(
            red.at[m], red.at[m], ssem.at[5], rmisc.at[1], device_id=dev(d, mm), device_id_type=MESH
        ).start()
    landed(red, 5, rmisc.at[1], 2 * nx - 1)
    tot = red[0]
    for k in range(1, 2 * nx):
        tot = tot + red[k]
    value = tot[1:2] * lax.rsqrt(tot[0:1] * (1.0 / D) + epsilon)
    val_ref[...] = value
    outs[1].start()
    old = old_ref[...]
    returns = adv_ref[...] + old
    clipped = old + jnp.clip(value - old, -clip_range, clip_range)
    terms = jnp.maximum((value - returns) ** 2, (clipped - returns) ** 2)
    part = jnp.sum(terms, axis=1, keepdims=True)

    lz[d] = jnp.broadcast_to(part, lz.shape[1:])
    far = sorted(range(nz), key=lambda k: -min(k, nz - k))
    for k in far:
        for yy in (yo, yl):
            for cc in (co, c):
                if k == 0 and yy is yl and cc is c:
                    continue
                pltpu.make_async_remote_copy(
                    lz.at[d], lz.at[d], ssem.at[6], rmisc.at[2],
                    device_id=dev(dpi(yy, zat(k), cc), m), device_id_type=MESH,
                ).start()

    landed(lz, 6, rmisc.at[2], ndp - 1)
    total = lz[0]
    for k in range(1, ndp):
        total = total + lz[k]
    loss_ref[...] = total * (0.5 / (T * ndp))
    outs[2].start()

    SQ.drain(2 * (ndp - 1))
    SKV.drain(ndp - 1)
    SO.drain(ndp - 1)

    def drain(buf, sem, count):
        ref = buf.at[pl.ds(0, count)]
        pltpu.make_async_remote_copy(
            ref, ref, ssem.at[sem], rmisc.at[1], device_id=sib, device_id_type=MESH
        ).wait_send()

    drain(att, 3, 14 * heads)
    drain(gae, 4, nwin - 1)
    drain(red, 5, 2 * nx - 1)
    drain(lz, 6, ndp - 1)
    for copy in outs:
        copy.wait()


def solution(mesh):
    ndp, nmp = mesh.shape["dp"], mesh.shape["mp"]
    nz, nx = ndp // 4, nmp // 2
    nwin = 5

    def body(hidden_in, w_query, w_key, w_value, w_out, value_weight, rewards, old_values, lengths, terminal):
        T, D = hidden_in.shape
        R, FQ = w_query.shape
        FK = w_key.shape[1]
        heads = FQ // HEAD
        nl = lengths.shape[0]
        half = HEAD // 2
        freq = rope_base ** (-jnp.arange(half, dtype=F32) * 2.0 / HEAD)
        upper = (jnp.arange(HEAD, dtype=jnp.int32) // half) * (T // 2)
        positions = lax.axis_index("dp") * T + jnp.arange(T // 2, dtype=jnp.int32)
        angles = (positions[:, None] + upper[None, :]).astype(F32) * jnp.concatenate([freq, freq])[None, :]
        cosine, sine = jnp.cos(angles), jnp.sin(angles)
        any_ = pl.BlockSpec(memory_space=pl.ANY)
        dma = pltpu.SemaphoreType.DMA
        out, loss = pl.pallas_call(
            functools.partial(kernel, nz, nx),
            out_shape=(
                jax.ShapeDtypeStruct((2, 1, T), F32),
                jax.ShapeDtypeStruct((1, 128), F32),
            ),
            in_specs=[any_] * 12,
            out_specs=(any_, any_),
            scratch_shapes=[
                pltpu.VMEM((T // 2, HEAD), F32),
                pltpu.VMEM((T // 2, HEAD), F32),
                pltpu.VMEM((1, FQ), F32),
                pltpu.VMEM((1, T), F32),
                pltpu.VMEM((1, T), F32),
                pltpu.VMEM((1, nl), jnp.int32),
                pltpu.VMEM((1, nl), jnp.int32),
                pltpu.VMEM((1, T), F32),
                pltpu.VMEM((1, T), F32),
                pltpu.VMEM((1, 128), F32),
                pltpu.VMEM((T, D), BF16),
                pltpu.VMEM((T, FQ), BF16),
                pltpu.VMEM((D, FQ), BF16),
                pltpu.VMEM((D, 2 * FK), BF16),
                pltpu.VMEM((D, FQ), BF16),
                pltpu.VMEM((nmp * 2 * heads, T // 2, HEAD), BF16),
                pltpu.VMEM((T, FQ), F32),
                pltpu.VMEM((T, 2 * FK), F32),
                pltpu.VMEM((heads, T, HEAD), BF16),
                pltpu.VMEM((T, HEAD), BF16),
                pltpu.VMEM((T, HEAD), BF16),
                pltpu.VMEM((T, T), F32),
                pltpu.VMEM((T, FQ), F32),
                pltpu.VMEM((16, T), F32),
                pltpu.VMEM((nwin, 2, T), F32),
                pltpu.VMEM((nmp, 2, T), F32),
                pltpu.VMEM((ndp, 1, 128), F32),
                dma((16,)),
                dma((9 * nz // 2 + 2,)),
                dma((5 * nz // 2 + 2,)),
                dma((2 * nz + 2,)),
                dma((att_sems(heads),)),
                dma((3,)),
                dma((7,)),
            ],
            compiler_params=pltpu.CompilerParams(collective_id=0, has_side_effects=True),
        )(
            hidden_in, w_query, w_key, w_value, w_out, cosine, sine,
            value_weight.reshape(1, FQ), rewards.reshape(1, T), old_values.reshape(1, T),
            lengths.reshape(1, nl), terminal.reshape(1, nl),
        )
        return out[0, 0], out[1, 0], loss[0, 0]

    return jax.shard_map(
        body,
        mesh=mesh,
        in_specs=(
            P("dp", None), P("dp", "mp"), P("dp", "mp"), P("dp", "mp"), P("dp", "mp"),
            P("mp"), P("dp"), P("dp"), P(), P(),
        ),
        out_specs=(P("dp"), P("dp"), P()),
        check_vma=False,
    )
```

```python
import functools
import math

import jax
import jax.numpy as jnp
from jax import lax
from jax.experimental import pallas as pl
from jax.experimental.pallas import tpu as pltpu
from jax.sharding import PartitionSpec as P

HEAD = 128
discount = 0.999
trace_decay = 0.997
clip_range = 0.2
epsilon = 1e-05
rope_base = 500000.0

MESH = pl.DeviceIdType.MESH
F32 = jnp.float32
BF16 = jnp.bfloat16


CUT = 3


def att_numbers(heads):
    bulk, own = [0] * 5, {}
    kinds = ["near", "two", "y", "far", "last"]
    table = {}
    for kind, k, p in [(kind, k, p) for kind in kinds for k in ((-1, 1) if kind in ("near", "far") else (0,)) for p in range(2 * heads)]:
        turn = k == -1
        passed = {
            "near": turn or p < CUT, "two": p < CUT, "y": p >= CUT, "far": turn and p >= CUT, "last": False
        }[kind]
        if passed:
            table[kind, k, p] = 5 + len(own)
            own[kind, k, p] = True
        else:
            table[kind, k, p] = kinds.index(kind)
            bulk[kinds.index(kind)] += 1
    return (lambda kind, k, p: table[kind, k, p]), bulk


def att_sems(heads):
    number, bulk = att_numbers(heads)
    return 1 + max(number(kind, k, p) for kind, k in (("near", -1), ("near", 1), ("two", 0), ("y", 0), ("far", -1), ("far", 1), ("last", 0)) for p in range(2 * heads))


def kernel(
    nz, nx,
    hid_hbm, wq_hbm, wk_hbm, wv_hbm, wo_hbm, fr_hbm, vw_hbm, rew_hbm, old_hbm, len_hbm, term_hbm,
    out_hbm, loss_hbm,
    cs_ref, sn_ref, fr_ref, vw_ref, rew_ref, old_ref, len_ref, term_ref, val_ref, adv_ref, loss_ref,
    hid, hown, wq, wkv, wo, att, accq, acckv, qs, ks, vs, bias, acco, rows_s, gae, red, lz,
    lsem, rq, rkv, ro, ratt, rmisc, ssem,
):
    D = hid.shape[1]
    T = hid.shape[0]
    R = wq_hbm.shape[0]
    FQ = wq_hbm.shape[1]
    FK = wk_hbm.shape[1]
    heads = FQ // HEAD
    nwin = gae.shape[0]
    ndp = 4 * nz
    half = nz // 2

    d = lax.axis_index("dp")
    m = lax.axis_index("mp")
    c = lax.rem(d, 2)
    z = lax.rem(d // 2, nz)
    yl = d // (2 * nz)
    yo = 1 - yl
    co = 1 - c
    xh = lax.rem(m, nx)
    yh = m // nx

    def dpi(yy, zz, cc):
        return (yy * nz + zz) * 2 + cc

    def zat(k):
        return lax.rem(z + (2 * nz + k), nz)

    def mpi(hh, k):
        return hh * nx + lax.rem(xh + (2 * nx + k), nx)

    def dev(dd, mm):
        return {"dp": dd, "mp": mm}

    sib = dev(dpi(yl, z, co), m)
    ypart = dev(dpi(yo, z, c), m)

    def zdev(k):
        return dev(dpi(yl, zat(k), c), m)

    def wslot(buf, idx, n, count=1):
        return buf.at[pl.ds(pl.multiple_of(idx * n, n), count * n)]

    class Stream:
        def __init__(self, buf, send, n):
            self.buf, self.sendsem, self.n = buf, send, n

        def copy(self, ref, sem, to):
            return pltpu.make_async_remote_copy(ref, ref, ssem.at[self.sendsem], sem, device_id=to, device_id_type=MESH)

        def send(self, idx, sem, to):
            self.copy(wslot(self.buf, idx, self.n), sem, to).start()

        def wait(self, sem, count=1):
            self.copy(wslot(self.buf, 0, self.n, count), sem, sib).wait_recv()

        def drain(self, count):
            self.copy(wslot(self.buf, 0, self.n, count), ssem.at[self.sendsem], sib).wait_send()

    SQ = Stream(wq, 0, R // 2)
    SKV = Stream(wkv, 1, R)
    SO = Stream(wo, 2, R)

    own = pl.ds(pl.multiple_of(d * R, R), R)
    copies = [
        pltpu.make_async_copy(wk_hbm, wkv.at[own, pl.ds(0, FK)], lsem.at[0]),
        pltpu.make_async_copy(wv_hbm, wkv.at[own, pl.ds(FK, FK)], lsem.at[1]),
        pltpu.make_async_copy(wq_hbm, wq.at[own], lsem.at[2]),
        pltpu.make_async_copy(wo_hbm, wo.at[own], lsem.at[3]),
        pltpu.make_async_copy(hid_hbm, hid, lsem.at[4]),
        pltpu.make_async_copy(
            hid_hbm.at[:, pl.ds(pl.multiple_of(m * FQ, FQ), FQ)], hown, lsem.at[5]
        ),
    ]
    small = [
        pltpu.make_async_copy(src, dst, lsem.at[6 + i])
        for i, (src, dst) in enumerate([
            (rew_hbm, rew_ref), (old_hbm, old_ref), (len_hbm, len_ref), (term_hbm, term_ref),
            (vw_hbm, vw_ref), (fr_hbm, fr_ref),
        ])
    ]
    outs = [
        pltpu.make_async_copy(src, dst, lsem.at[12 + i])
        for i, (src, dst) in enumerate([(adv_ref, out_hbm.at[1]), (val_ref, out_hbm.at[0]), (loss_ref, loss_hbm)])
    ]
    for copy in copies[:3]:
        copy.start()

    kappa = math.log(discount * trace_decay)

    nl = len_ref.shape[1]

    def ends():
        si = lax.broadcasted_iota(jnp.int32, (nl, nl), 0)
        li = lax.broadcasted_iota(jnp.int32, (nl, nl), 1)
        lens = len_ref[...].astype(F32)
        ends_col = jnp.sum(jnp.where(li <= si, lens, 0.0), axis=1, keepdims=True)
        return si, li, ends_col

    base = (d * T).astype(F32)
    lane = lax.broadcasted_iota(jnp.int32, (1, T), 1)

    def landed(buf, send, sem, count):
        ref = buf.at[pl.ds(0, count)]
        pltpu.make_async_remote_copy(ref, ref, ssem.at[send], sem, device_id=sib, device_id_type=MESH).wait_recv()

    def first_marks():
        si, li, ends_col = ends()
        rows_s[pl.ds(6, 1), pl.ds(0, nl)] = jnp.sum(jnp.where(li == si, ends_col, 0.0), axis=0, keepdims=True)
        pos = base + lane.astype(F32)
        rows_s[pl.ds(0, 1), :] = jnp.sum(jnp.where(ends_col <= pos, 1.0, 0.0), axis=0, keepdims=True)

    xp, xm = dev(d, mpi(yh, 1)), dev(d, mpi(yh, -1))

    def away(p, k=1):
        return k * (1 - 2 * lax.rem(c + p, 2))

    def xdev(k):
        return dev(d, mpi(yh, k))

    yx = dev(d, mpi(1 - yh, 0))
    peers = [zdev(1), zdev(-1), sib, ypart, xp, xm, yx]
    mpeers = [lax.rem(m + k, 2 * nx) for k in range(1, 2 * nx)]
    barrier = pltpu.get_barrier_semaphore()
    for peer in peers:
        pl.semaphore_signal(barrier, inc=1, device_id=peer, device_id_type=MESH)
    for copy in copies[4:] + small + copies[3:4]:
        copy.start()
    for copy in copies[:3]:
        copy.wait()
    pl.semaphore_wait(barrier, len(peers))

    sgn = 2 * c - 1
    onward = zdev(sgn)

    other, theirs, both = dpi(yo, z, c), dpi(yl, z, co), dpi(yo, z, co)

    def q_ring(s, n, i):
        return rq.at[(s - 1) * 4 + n * 2 + i]

    def q_cross(k, n, i):
        return rq.at[4 * half - 2 + k * 4 + n * 2 + i]

    def q_sib(k):
        return rq.at[8 * half + k]

    def kv_ring(s, n, r):
        return rkv.at[(s - 1) * 4 + n * 2 + r]

    def kv_sib(k):
        return rkv.at[4 * half - 2 + k]

    def o_ring(s, n, r):
        return ro.at[(s - 1) * 4 + n * 2 + r]

    KV_Y, KV_THEIRS, KV_BOTH = (rkv.at[5 * half - 1 + k] for k in range(3))
    O_Y, O_THEIRS, O_BOTH, O_SIB = (ro.at[4 * half - 2 + k] for k in range(4))
    Q_THEIRS = rq.at[9 * half + 1]

    def core_of(n):
        return c if n == 0 else co

    def zat_(k):
        return lax.rem(z + 2 * nz + k, nz)

    def nothing():
        pass

    def kv_pass(s, zo, n, r, on):
        ik = dpi(yl if r == 0 else yo, zo, core_of(n))
        SKV.wait(kv_ring(s, n, r))
        if on:
            SKV.send(ik, kv_ring(s + 1, n, r), onward)
        SKV.send(ik, kv_sib(s - 1), sib)

    def across(k, n, i):
        iq = dpi(yo, zat_(-sgn * k), core_of(n)) * 2 + i
        SQ.wait(q_cross(k, n, i))
        SQ.send(iq, q_sib(k), sib)

    def qkv_step(s, pieces, cores=(0, 1), out=(0, 1)):
        zo = zat_(-sgn * s)
        todo = list(pieces)
        first = isinstance(s, int) and s == 1
        crossing = [(n, i) for n in ((0,) if first else (0, 1)) for i in (0, 1)]

        def work():
            if todo:
                todo.pop(0)()

        def cross_next():
            if crossing:
                across(s - 1, *crossing.pop(0))

        for n in cores:
            for i in (0, 1):
                iq = dpi(yl, zo, core_of(n)) * 2 + i
                SQ.wait(q_ring(s, n, i))
                if n in out:
                    SQ.send(iq, q_ring(s + 1, n, i), onward)
                SQ.send(iq, q_cross(s, n, i), ypart)
                SQ.send(iq, q_sib(s), sib)
                work()
            kv_pass(s, zo, n, 0, n in out)
            cross_next()
            work()
        for n in cores:
            kv_pass(s, zo, n, 1, n in out)
            cross_next()
            work()
        while crossing:
            cross_next()
        while todo:
            work()

    def wo_first():
        SO.send(d, o_ring(1, 0, 0), onward)
        SO.wait(O_THEIRS)
        SO.send(theirs, o_ring(1, 1, 0), onward)
        SO.wait(O_Y)
        SO.send(other, o_ring(1, 0, 1), onward)
        SO.send(other, O_BOTH, sib)
        SO.wait(O_BOTH)
        SO.send(both, o_ring(1, 1, 1), onward)

    def wo_step(s):
        zo = zat_(-sgn * s)
        for n in (0,) if s == half else (0, 1):
            for r, yy in enumerate((yl, yo)):
                io = dpi(yy, zo, core_of(n))
                SO.wait(o_ring(s, n, r))
                if s < half - 1 or (s == half - 1 and n == 0):
                    SO.send(io, o_ring(s + 1, n, r), onward)
                SO.send(io, O_SIB, sib)

    def norm_rows(i, _):
        rr = pl.ds(pl.multiple_of(i * 32, 32), 32)
        x = hid[rr, :].astype(F32)
        ms = jnp.sum(x * x, axis=1, keepdims=True) * (1.0 / D)
        hid[rr, :] = (x * lax.rsqrt(ms + epsilon)).astype(BF16)
        return 0

    def rows_of(zz):
        return [pl.ds(pl.multiple_of(dpi(yy, zz, 0) * R, 2 * R), 2 * R) for yy in (0, 1)]

    def mm_q(zz):
        lhs = jnp.concatenate([hid[:, r] for r in rows_of(zz)], axis=1)
        rhs = jnp.concatenate([wq[r, :] for r in rows_of(zz)], axis=0)
        accq[...] += jnp.dot(lhs, rhs, preferred_element_type=F32)

    def mm_kv(zz):
        lhs = jnp.concatenate([hid[:, r] for r in rows_of(zz)], axis=1)
        rhs = jnp.concatenate([wkv[r, :] for r in rows_of(zz)], axis=0)
        acckv[...] += jnp.dot(lhs, rhs, preferred_element_type=F32)

    def opp_q(k):
        SQ.wait(q_sib(k), 8)
        mm_q(zat_(sgn * k))

    def opp_kv(k):
        SKV.wait(kv_sib(k - 1), 4)
        mm_kv(zat_(sgn * k))

    NB = 64

    def block_of(r):
        sub = r * NB + lax.broadcasted_iota(jnp.int32, (NB, 1), 0)
        posc = base + sub.astype(F32)
        epc = jnp.sum(jnp.where(rows_s[pl.ds(6, 1), pl.ds(0, nl)] <= posc, 1.0, 0.0), axis=1, keepdims=True)
        ll = lax.broadcasted_iota(jnp.int32, (NB, T), 1)
        ss = r * NB + lax.broadcasted_iota(jnp.int32, (NB, T), 0)
        return sub, epc, ll, ss

    def bias_rows(r, _):
        sub, epc, ll, ss = block_of(r)
        same = rows_s[pl.ds(0, 1), :] == epc
        bias[pl.ds(pl.multiple_of(r * NB, NB), NB), :] = jnp.where((ll <= ss) & same, 0.0, -1e30)
        return 0

    def angle_rows(r, _):
        n = 32
        rr = lax.broadcasted_iota(jnp.int32, (n, HEAD), 0)
        upper = jnp.where(lax.broadcasted_iota(jnp.int32, (n, HEAD), 1) < HEAD // 2, 0, T // 2)
        angles = (rr + upper + (d * T + r * n)).astype(F32) * fr_ref[...]
        at = pl.ds(pl.multiple_of(r * n, n), n)
        cs_ref[at, :] = jnp.cos(angles)
        sn_ref[at, :] = jnp.sin(angles)
        return 0

    def gae_send():
        for k in range(1, nwin):
            pltpu.make_async_remote_copy(
                gae.at[0], gae.at[k], ssem.at[4], rmisc.at[0],
                device_id=dev(lax.rem(d + ndp - k, ndp), m), device_id_type=MESH,
            ).start()

    def advantages():
        landed(gae, 4, rmisc.at[0], nwin - 1)
        si, li, ends_col = ends()
        term_col = jnp.sum(jnp.where(li == si, term_ref[...].astype(F32), 0.0), axis=1, keepdims=True)
        for k in range(nwin):
            pos = base + (lane + k * T).astype(F32)
            ep = jnp.sum(jnp.where(ends_col <= pos, 1.0, 0.0), axis=0, keepdims=True)
            hit = (ends_col - 1.0) == pos
            fin = jnp.sum(jnp.where(hit, 1.0, 0.0), axis=0, keepdims=True)
            stp = jnp.sum(jnp.where(hit, term_col, 0.0), axis=0, keepdims=True)
            rew = gae[k, pl.ds(0, 1), :]
            old = gae[k, pl.ds(1, 1), :]
            nxt = pltpu.roll(old, T - 1, 1)
            if k + 1 < nwin:
                nxt = jnp.where(lane == T - 1, gae[k + 1, pl.ds(1, 1), :][:, :1], nxt)
            booted = jnp.where(fin > 0.0, (1.0 - stp) * old, nxt)
            delta = rew + discount * booted - old
            rows_s[pl.ds(k, 1), :] = ep
            rows_s[pl.ds(8 + k, 1), :] = delta * jnp.exp((lane + k * T).astype(F32) * kappa)

        def rowblock(r, advr):
            sub, epc, ll, ss = block_of(r)
            same = rows_s[pl.ds(0, 1), :] == epc
            tot = jnp.where((ll >= ss) & same, rows_s[pl.ds(8, 1), :], 0.0)
            for k in range(1, nwin):
                tot += jnp.where(rows_s[pl.ds(k, 1), :] == epc, rows_s[pl.ds(8 + k, 1), :], 0.0)
            col = jnp.sum(tot, axis=1, keepdims=True) * jnp.exp(sub.astype(F32) * (-kappa))
            return advr + jnp.sum(jnp.where(ll == ss, col, 0.0), axis=0, keepdims=True)

        adv_ref[...] = lax.fori_loop(0, T // NB, rowblock, jnp.zeros((1, T), F32))
        outs[0].start()

    SKV.send(d, KV_Y, ypart)
    for i in (0, 1):
        SQ.send(2 * d + i, Q_THEIRS, sib)
    SKV.send(d, KV_THEIRS, sib)
    for i in (0, 1):
        SQ.send(2 * d + i, q_ring(1, 0, i), onward)
    SKV.send(d, kv_ring(1, 0, 0), onward)
    for i in (0, 1):
        SQ.send(2 * d + i, q_cross(0, 0, i), ypart)
    SQ.wait(Q_THEIRS, 2)
    for i in (0, 1):
        SQ.send(2 * theirs + i, q_ring(1, 1, i), onward)
    SKV.wait(KV_THEIRS)
    SKV.send(theirs, kv_ring(1, 1, 0), onward)
    accq[...] = jnp.zeros_like(accq)
    acckv[...] = jnp.zeros_like(acckv)
    for copy in small + copies[4:5]:
        copy.wait()
    gae[0, pl.ds(0, 1), :] = rew_ref[...]
    gae[0, pl.ds(1, 1), :] = old_ref[...]
    first_marks()
    lax.fori_loop(0, 4, norm_rows, 0)
    def norms(lo, hi):
        return functools.partial(lax.fori_loop, lo, hi, norm_rows, 0)

    def other_kv():
        SKV.wait(KV_Y)
        SKV.send(other, kv_ring(1, 0, 1), onward)
        SKV.send(other, KV_BOTH, sib)

    def both_kv():
        SKV.wait(KV_BOTH)
        SKV.send(both, kv_ring(1, 1, 1), onward)

    qkv_step(1, [norms(4, 5), other_kv, both_kv, norms(5, 6), norms(6, 7), norms(7, 8), norms(8, 9), norms(9, 10)])
    def biases(lo, hi):
        return functools.partial(lax.fori_loop, lo, hi, bias_rows, 0)

    def own_q():
        SQ.wait(q_sib(0), 2)
        mm_q(z)

    def own_kv():
        mm_kv(z)

    qkv_step(2, [norms(10, 11), norms(11, 12), norms(12, 13), norms(13, 14), norms(14, 15), norms(15, 16), own_kv, own_q])
    def pieces_at(s):
        k = s - 2
        zm = zat_(-sgn * k)
        return [nothing, lambda: mm_q(zm), nothing, lambda: mm_kv(zm), nothing, lambda: opp_q(k), nothing, lambda: opp_kv(k)]

    share = T // NB // (half - 4)

    def mid(s, _):
        extra = pieces_at(s)
        extra[0] = functools.partial(lax.fori_loop, (s - 3) * share, (s - 2) * share, bias_rows, 0)
        extra[2] = lambda: angle_rows((s - 3) * 2, 0)
        extra[4] = lambda: angle_rows((s - 3) * 2 + 1, 0)
        qkv_step(s, extra)
        return 0

    lax.fori_loop(3, half - 1, mid, 0)
    copies[3].wait()
    SO.send(d, O_THEIRS, sib)
    SO.send(d, O_Y, ypart)
    qkv_step(half - 1, pieces_at(half - 1), out=(0,))
    wo_first()
    qkv_step(half, pieces_at(half), cores=(0,), out=())
    mm_kv(zat_(-sgn * (half - 1)))
    mm_q(zat_(-sgn * (half - 1)))
    for i in (0, 1):
        across(half, 0, i)
    opp_kv(half - 1)
    opp_q(half - 1)
    SKV.wait(kv_sib(half - 1), 2)
    mm_kv(zat_(half))
    wo_step(1)
    SQ.wait(q_sib(half), 4)
    mm_q(zat_(half))

    low = lax.broadcasted_iota(jnp.int32, (T // 2, HEAD), 1) < HEAD // 2

    def spread(ref, sign):
        table = ref[...]
        turned = pltpu.roll(table, HEAD // 2, 1)
        first, second = jnp.where(low, table, turned), jnp.where(low, turned, table)
        if sign:
            first, second = jnp.where(low, -first, first), jnp.where(low, -second, second)
        return first, second

    cosines, sines = spread(cs_ref, False), spread(sn_ref, True)

    def rope(load, store):
        for n in (0, 1):
            x = load(slice(n * T // 2, (n + 1) * T // 2))
            store(slice(n * T // 2, (n + 1) * T // 2), (x * cosines[n] + pltpu.roll(x, HEAD // 2, 1) * sines[n]).astype(BF16))

    def put_q(h):
        def store(r, x):
            qs[h, r, :] = x
        return store

    def put_k(r, x):
        ks[r, :] = x

    def rope_q(h):
        rope(lambda r: accq[r, h * HEAD:(h + 1) * HEAD], put_q(h))

    rope(lambda r: acckv[r, :FK], put_k)
    vs[...] = acckv[:, FK:].astype(BF16)

    scale = 1.0 / HEAD**0.5

    number, bulk = att_numbers(heads)

    def att_copy(o, p, kind, k, to):
        i = o * (2 * heads) + p
        n = number(kind, k, p)
        return pltpu.make_async_remote_copy(
            att.at[i], att.at[i], ssem.at[3], ratt.at[n], device_id=to, device_id_type=MESH
        )

    def att_send(o, p, kind, k, to):
        att_copy(o, p, kind, k, to).start()

    def att_wait(o, p, kind, k):
        if number(kind, k, p) >= len(bulk):
            att_copy(o, p, kind, k, sib).wait_recv()

    def att_rest(n):
        landed(att, 3, ratt.at[n], bulk[n])

    QB = 128

    def piece_send(p):
        att_send(m, p, "near", -1, xdev(away(p)))
        att_send(m, p, "near", 1, xdev(away(p, -1)))
        att_send(m, p, "y", 0, yx)

    def head_step(h):
        for i in range(T // QB):
            n = (i + 1) * QB
            sc = lax.dot_general(
                qs[h, i * QB:n, :], ks[:n, :], (((1,), (1,)), ((), ())), preferred_element_type=F32
            ) * scale + bias[i * QB:n, :n]
            big = jnp.max(sc, axis=1, keepdims=True)
            ex = jnp.exp(sc - big)
            pr = (ex / jnp.sum(ex, axis=1, keepdims=True)).astype(BF16)
            out = jnp.dot(pr, vs[:n, :], preferred_element_type=F32)
            r = 2 * i // (T // QB)
            low_row = i * QB - r * (T // 2)
            att[m * (2 * heads) + 2 * h + r, low_row:low_row + QB, :] = out.astype(BF16)
            if (i + 1) * 2 % (T // QB) == 0:
                piece_send(2 * h + r)

    rope_q(0)
    head_step(0)
    rope_q(1)
    head_step(1)
    gae_send()
    rope_q(2)
    head_step(2)
    wo_step(2)
    for h in range(3, heads):
        rope_q(h)
        head_step(h)

    cut = CUT

    def relay_near(p):
        for k in (-1, 1):
            o = mpi(yh, away(p, k))
            att_wait(o, p, "near", k)
            if k == -1:
                att_send(o, p, "two", 0, xdev(away(p)))
            if p < cut:
                att_send(o, p, "far", k, yx)

    def relay_two(p):
        o = mpi(yh, 2)
        att_wait(o, p, "two", 0)
        if p < cut:
            att_send(o, p, "last", 0, yx)

    def relay_y(p):
        o = mpi(1 - yh, 0)
        att_wait(o, p, "y", 0)
        if p >= cut:
            att_send(o, p, "far", -1, xdev(away(p)))
            att_send(o, p, "far", 1, xdev(away(p, -1)))

    def relay_far(p):
        for k in (-1, 1):
            o = mpi(1 - yh, away(p, k))
            att_wait(o, p, "far", k)
            if p >= cut and k == -1:
                att_send(o, p, "last", 0, xdev(away(p)))

    for p in range(cut):
        relay_near(p)
    wo_step(3)
    advantages()
    wo_step(4)
    for p in range(cut, 2 * heads):
        relay_near(p)
        relay_y(p)
    wo_step(5)
    for p in range(cut):
        relay_two(p)
    wo_step(6)
    relay_far(3)
    relay_far(4)
    wo_step(7)
    relay_far(5)
    relay_far(6)
    wo_step(8)
    relay_far(7)

    SO.wait(O_SIB, 4 * half - 2)
    def project(o):
        r0 = pl.ds(pl.multiple_of(o * FQ, FQ), FQ)
        for r in (0, 1):
            lhs = jnp.concatenate([att[o * (2 * heads) + 2 * h + r] for h in range(heads)], axis=1)
            acco[r * T // 2:(r + 1) * T // 2, :] += jnp.dot(lhs, wo[r0, :], preferred_element_type=F32)

    copies[5].wait()
    acco[...] = hown[...].astype(F32)
    project(m)
    att_rest(0)
    project(mpi(yh, 1))
    project(mpi(yh, -1))
    att_rest(1)
    project(mpi(yh, 2))
    att_rest(2)
    project(mpi(1 - yh, 0))
    att_rest(3)
    project(mpi(1 - yh, 1))
    project(mpi(1 - yh, -1))
    att_rest(4)
    project(mpi(1 - yh, 2))

    def sums(r, carry):
        n = 64
        x = acco[pl.ds(pl.multiple_of(r * n, n), n), :]
        ll = lax.broadcasted_iota(jnp.int32, (n, T), 1)
        ss = r * n + lax.broadcasted_iota(jnp.int32, (n, T), 0)
        sq = jnp.sum(x * x, axis=1, keepdims=True)
        hs = jnp.sum(x * vw_ref[...], axis=1, keepdims=True)
        a, b = carry
        a = a + jnp.sum(jnp.where(ll == ss, sq, 0.0), axis=0, keepdims=True)
        b = b + jnp.sum(jnp.where(ll == ss, hs, 0.0), axis=0, keepdims=True)
        return a, b

    zero = jnp.zeros((1, T), F32)
    sq, hs = lax.fori_loop(0, T // 64, sums, (zero, zero), unroll=True)
    red[m, pl.ds(0, 1), :] = sq
    red[m, pl.ds(1, 1), :] = hs
    for mm in mpeers:
        pltpu.make_async_remote_copy(
            red.at[m], red.at[m], ssem.at[5], rmisc.at[1], device_id=dev(d, mm), device_id_type=MESH
        ).start()
    landed(red, 5, rmisc.at[1], 2 * nx - 1)
    tot = red[0]
    for k in range(1, 2 * nx):
        tot = tot + red[k]
    value = tot[1:2] * lax.rsqrt(tot[0:1] * (1.0 / D) + epsilon)
    val_ref[...] = value
    outs[1].start()
    old = old_ref[...]
    returns = adv_ref[...] + old
    clipped = old + jnp.clip(value - old, -clip_range, clip_range)
    terms = jnp.maximum((value - returns) ** 2, (clipped - returns) ** 2)
    part = jnp.sum(terms, axis=1, keepdims=True)

    lz[d] = jnp.broadcast_to(part, lz.shape[1:])
    far = sorted(range(nz), key=lambda k: -min(k, nz - k))
    for k in far:
        for yy in (yo, yl):
            for cc in (co, c):
                if k == 0 and yy is yl and cc is c:
                    continue
                pltpu.make_async_remote_copy(
                    lz.at[d], lz.at[d], ssem.at[6], rmisc.at[2],
                    device_id=dev(dpi(yy, zat(k), cc), m), device_id_type=MESH,
                ).start()

    landed(lz, 6, rmisc.at[2], ndp - 1)
    total = lz[0]
    for k in range(1, ndp):
        total = total + lz[k]
    loss_ref[...] = total * (0.5 / (T * ndp))
    outs[2].start()

    SQ.drain(2 * (ndp - 1))
    SKV.drain(ndp - 1)
    SO.drain(ndp - 1)

    def drain(buf, sem, count):
        ref = buf.at[pl.ds(0, count)]
        pltpu.make_async_remote_copy(
            ref, ref, ssem.at[sem], rmisc.at[1], device_id=sib, device_id_type=MESH
        ).wait_send()

    drain(att, 3, 14 * heads)
    drain(gae, 4, nwin - 1)
    drain(red, 5, 2 * nx - 1)
    drain(lz, 6, ndp - 1)
    for copy in outs:
        copy.wait()


def solution(mesh):
    ndp, nmp = mesh.shape["dp"], mesh.shape["mp"]
    nz, nx = ndp // 4, nmp // 2
    nwin = 5

    def body(hidden_in, w_query, w_key, w_value, w_out, value_weight, rewards, old_values, lengths, terminal):
        T, D = hidden_in.shape
        R, FQ = w_query.shape
        FK = w_key.shape[1]
        heads = FQ // HEAD
        nl = lengths.shape[0]
        half = HEAD // 2
        freq = rope_base ** (-(jnp.arange(HEAD, dtype=jnp.int32) % half).astype(F32) * 2.0 / HEAD)
        any_ = pl.BlockSpec(memory_space=pl.ANY)
        dma = pltpu.SemaphoreType.DMA
        out, loss = pl.pallas_call(
            functools.partial(kernel, nz, nx),
            out_shape=(
                jax.ShapeDtypeStruct((2, 1, T), F32),
                jax.ShapeDtypeStruct((1, 128), F32),
            ),
            in_specs=[any_] * 11,
            out_specs=(any_, any_),
            scratch_shapes=[
                pltpu.VMEM((T // 2, HEAD), F32),
                pltpu.VMEM((T // 2, HEAD), F32),
                pltpu.VMEM((1, HEAD), F32),
                pltpu.VMEM((1, FQ), F32),
                pltpu.VMEM((1, T), F32),
                pltpu.VMEM((1, T), F32),
                pltpu.VMEM((1, nl), jnp.int32),
                pltpu.VMEM((1, nl), jnp.int32),
                pltpu.VMEM((1, T), F32),
                pltpu.VMEM((1, T), F32),
                pltpu.VMEM((1, 128), F32),
                pltpu.VMEM((T, D), BF16),
                pltpu.VMEM((T, FQ), BF16),
                pltpu.VMEM((D, FQ), BF16),
                pltpu.VMEM((D, 2 * FK), BF16),
                pltpu.VMEM((D, FQ), BF16),
                pltpu.VMEM((nmp * 2 * heads, T // 2, HEAD), BF16),
                pltpu.VMEM((T, FQ), F32),
                pltpu.VMEM((T, 2 * FK), F32),
                pltpu.VMEM((heads, T, HEAD), BF16),
                pltpu.VMEM((T, HEAD), BF16),
                pltpu.VMEM((T, HEAD), BF16),
                pltpu.VMEM((T, T), F32),
                pltpu.VMEM((T, FQ), F32),
                pltpu.VMEM((16, T), F32),
                pltpu.VMEM((nwin, 2, T), F32),
                pltpu.VMEM((nmp, 2, T), F32),
                pltpu.VMEM((ndp, 1, 128), F32),
                dma((15,)),
                dma((9 * nz // 2 + 2,)),
                dma((5 * nz // 2 + 2,)),
                dma((2 * nz + 2,)),
                dma((att_sems(heads),)),
                dma((3,)),
                dma((7,)),
            ],
            compiler_params=pltpu.CompilerParams(collective_id=0, has_side_effects=True),
        )(
            hidden_in, w_query, w_key, w_value, w_out, freq.reshape(1, HEAD),
            value_weight.reshape(1, FQ), rewards.reshape(1, T), old_values.reshape(1, T),
            lengths.reshape(1, nl), terminal.reshape(1, nl),
        )
        return out[0, 0], out[1, 0], loss[0, 0]

    return jax.shard_map(
        body,
        mesh=mesh,
        in_specs=(
            P("dp", None), P("dp", "mp"), P("dp", "mp"), P("dp", "mp"), P("dp", "mp"),
            P("mp"), P("dp"), P("dp"), P(), P(),
        ),
        out_specs=(P("dp"), P("dp"), P()),
        check_vma=False,
    )
```

```python
import functools
import math

import jax
import jax.numpy as jnp
import numpy as np
from jax import lax
from jax.experimental import pallas as pl
from jax.experimental.pallas import tpu as pltpu
from jax.sharding import PartitionSpec as P

HEAD = 128
discount = 0.999
trace_decay = 0.997
clip_range = 0.2
epsilon = 1e-05
rope_base = 500000.0

MESH = pl.DeviceIdType.MESH
F32 = jnp.float32
BF16 = jnp.bfloat16


CUT = 3


def att_numbers(heads):
    bulk, own = [0] * 5, {}
    kinds = ["near", "two", "y", "far", "last"]
    table = {}
    for kind, k, p in [(kind, k, p) for kind in kinds for k in ((-1, 1) if kind in ("near", "far") else (0,)) for p in range(2 * heads)]:
        turn = k == -1
        passed = {
            "near": turn or p < CUT, "two": p < CUT, "y": p >= CUT, "far": turn and p >= CUT, "last": False
        }[kind]
        if passed:
            table[kind, k, p] = 5 + len(own)
            own[kind, k, p] = True
        else:
            table[kind, k, p] = kinds.index(kind)
            bulk[kinds.index(kind)] += 1
    return (lambda kind, k, p: table[kind, k, p]), bulk


def att_sems(heads):
    number, bulk = att_numbers(heads)
    return 1 + max(number(kind, k, p) for kind, k in (("near", -1), ("near", 1), ("two", 0), ("y", 0), ("far", -1), ("far", 1), ("last", 0)) for p in range(2 * heads))


def kernel(
    nz, nx,
    hid_hbm, wq_hbm, wk_hbm, wv_hbm, wo_hbm, fr_hbm, vw_hbm, rew_hbm, old_hbm, len_hbm, term_hbm,
    out_hbm, loss_hbm,
    cs_ref, sn_ref, fr_ref, vw_ref, rew_ref, old_ref, len_ref, term_ref, val_ref, adv_ref, loss_ref,
    hid, hown, wq, wkv, wo, att, accq, acckv, qs, ks, vs, bias, acco, rows_s, gae, red, lz,
    lsem, rq, rkv, ro, ratt, rmisc, ssem,
):
    D = hid.shape[1]
    T = hid.shape[0]
    R = wq_hbm.shape[0]
    FQ = wq_hbm.shape[1]
    FK = wk_hbm.shape[1]
    heads = FQ // HEAD
    nwin = gae.shape[0]
    ndp = 4 * nz
    half = nz // 2

    d = lax.axis_index("dp")
    m = lax.axis_index("mp")
    c = lax.rem(d, 2)
    z = lax.rem(d // 2, nz)
    yl = d // (2 * nz)
    yo = 1 - yl
    co = 1 - c
    xh = lax.rem(m, nx)
    yh = m // nx

    def dpi(yy, zz, cc):
        return (yy * nz + zz) * 2 + cc

    def zat(k):
        return lax.rem(z + (2 * nz + k), nz)

    def mpi(hh, k):
        return hh * nx + lax.rem(xh + (2 * nx + k), nx)

    def dev(dd, mm):
        return {"dp": dd, "mp": mm}

    sib = dev(dpi(yl, z, co), m)
    ypart = dev(dpi(yo, z, c), m)

    def zdev(k):
        return dev(dpi(yl, zat(k), c), m)

    def wslot(buf, idx, n, count=1):
        return buf.at[pl.ds(pl.multiple_of(idx * n, n), count * n)]

    class Stream:
        def __init__(self, buf, send, n):
            self.buf, self.sendsem, self.n = buf, send, n

        def copy(self, ref, sem, to):
            return pltpu.make_async_remote_copy(ref, ref, ssem.at[self.sendsem], sem, device_id=to, device_id_type=MESH)

        def send(self, idx, sem, to):
            self.copy(wslot(self.buf, idx, self.n), sem, to).start()

        def wait(self, sem, count=1):
            self.copy(wslot(self.buf, 0, self.n, count), sem, sib).wait_recv()

        def drain(self, count):
            self.copy(wslot(self.buf, 0, self.n, count), ssem.at[self.sendsem], sib).wait_send()

    SQ = Stream(wq, 0, R // 2)
    SKV = Stream(wkv, 1, R)
    SO = Stream(wo, 2, R)

    own = pl.ds(pl.multiple_of(d * R, R), R)
    copies = [
        pltpu.make_async_copy(wk_hbm, wkv.at[own, pl.ds(0, FK)], lsem.at[0]),
        pltpu.make_async_copy(wv_hbm, wkv.at[own, pl.ds(FK, FK)], lsem.at[1]),
        pltpu.make_async_copy(wq_hbm, wq.at[own], lsem.at[2]),
        pltpu.make_async_copy(wo_hbm, wo.at[own], lsem.at[3]),
        pltpu.make_async_copy(hid_hbm, hid, lsem.at[4]),
        pltpu.make_async_copy(
            hid_hbm.at[:, pl.ds(pl.multiple_of(m * FQ, FQ), FQ)], hown, lsem.at[5]
        ),
    ]
    small = [
        pltpu.make_async_copy(src, dst, lsem.at[6 + i])
        for i, (src, dst) in enumerate([
            (rew_hbm, rew_ref), (old_hbm, old_ref), (len_hbm, len_ref), (term_hbm, term_ref),
            (vw_hbm, vw_ref), (fr_hbm, fr_ref),
        ])
    ]
    outs = [
        pltpu.make_async_copy(src, dst, lsem.at[12 + i])
        for i, (src, dst) in enumerate([(adv_ref, out_hbm.at[1]), (val_ref, out_hbm.at[0]), (loss_ref, loss_hbm)])
    ]
    for copy in copies[:3]:
        copy.start()

    kappa = math.log(discount * trace_decay)

    nl = len_ref.shape[1]

    def ends():
        si = lax.broadcasted_iota(jnp.int32, (nl, nl), 0)
        li = lax.broadcasted_iota(jnp.int32, (nl, nl), 1)
        lens = len_ref[...].astype(F32)
        ends_col = jnp.sum(jnp.where(li <= si, lens, 0.0), axis=1, keepdims=True)
        return si, li, ends_col

    base = (d * T).astype(F32)
    lane = lax.broadcasted_iota(jnp.int32, (1, T), 1)

    def landed(buf, send, sem, count):
        ref = buf.at[pl.ds(0, count)]
        pltpu.make_async_remote_copy(ref, ref, ssem.at[send], sem, device_id=sib, device_id_type=MESH).wait_recv()

    def first_marks():
        si, li, ends_col = ends()
        rows_s[pl.ds(6, 1), pl.ds(0, nl)] = jnp.sum(jnp.where(li == si, ends_col, 0.0), axis=0, keepdims=True)
        pos = base + lane.astype(F32)
        rows_s[pl.ds(0, 1), :] = jnp.sum(jnp.where(ends_col <= pos, 1.0, 0.0), axis=0, keepdims=True)

    xp, xm = dev(d, mpi(yh, 1)), dev(d, mpi(yh, -1))

    def away(p, k=1):
        return k * (1 - 2 * lax.rem(c + p, 2))

    def xdev(k):
        return dev(d, mpi(yh, k))

    yx = dev(d, mpi(1 - yh, 0))
    peers = [zdev(1), zdev(-1), sib, ypart, xp, xm, yx]
    mpeers = [lax.rem(m + k, 2 * nx) for k in range(1, 2 * nx)]
    barrier = pltpu.get_barrier_semaphore()
    for peer in peers:
        pl.semaphore_signal(barrier, inc=1, device_id=peer, device_id_type=MESH)
    for copy in copies[4:] + small + copies[3:4]:
        copy.start()
    for copy in copies[:3]:
        copy.wait()
    pl.semaphore_wait(barrier, len(peers))

    sgn = 2 * c - 1
    onward = zdev(sgn)

    other, theirs, both = dpi(yo, z, c), dpi(yl, z, co), dpi(yo, z, co)

    def q_ring(s, n, i):
        return rq.at[(s - 1) * 4 + n * 2 + i]

    def q_cross(k, n, i):
        return rq.at[4 * half - 2 + k * 4 + n * 2 + i]

    def q_sib(k):
        return rq.at[8 * half + k]

    def kv_ring(s, n, r):
        return rkv.at[(s - 1) * 4 + n * 2 + r]

    def kv_sib(k):
        return rkv.at[4 * half - 2 + k]

    def o_ring(s, n, r):
        return ro.at[(s - 1) * 4 + n * 2 + r]

    KV_Y, KV_THEIRS, KV_BOTH = (rkv.at[5 * half - 1 + k] for k in range(3))
    O_Y, O_THEIRS, O_BOTH, O_SIB = (ro.at[4 * half - 2 + k] for k in range(4))
    Q_THEIRS = rq.at[9 * half + 1]

    def core_of(n):
        return c if n == 0 else co

    def zat_(k):
        return lax.rem(z + 2 * nz + k, nz)

    def nothing():
        pass

    def kv_pass(s, zo, n, r, on):
        ik = dpi(yl if r == 0 else yo, zo, core_of(n))
        SKV.wait(kv_ring(s, n, r))
        if on:
            SKV.send(ik, kv_ring(s + 1, n, r), onward)
        SKV.send(ik, kv_sib(s - 1), sib)

    def across(k, n, i):
        iq = dpi(yo, zat_(-sgn * k), core_of(n)) * 2 + i
        SQ.wait(q_cross(k, n, i))
        SQ.send(iq, q_sib(k), sib)

    def qkv_step(s, pieces, cores=(0, 1), out=(0, 1)):
        zo = zat_(-sgn * s)
        todo = list(pieces)
        first = isinstance(s, int) and s == 1
        crossing = [(n, i) for n in ((0,) if first else (0, 1)) for i in (0, 1)]

        def work():
            if todo:
                todo.pop(0)()

        def cross_next():
            if crossing:
                across(s - 1, *crossing.pop(0))

        for n in cores:
            for i in (0, 1):
                iq = dpi(yl, zo, core_of(n)) * 2 + i
                SQ.wait(q_ring(s, n, i))
                if n in out:
                    SQ.send(iq, q_ring(s + 1, n, i), onward)
                SQ.send(iq, q_cross(s, n, i), ypart)
                SQ.send(iq, q_sib(s), sib)
                work()
            kv_pass(s, zo, n, 0, n in out)
            cross_next()
            work()
        for n in cores:
            kv_pass(s, zo, n, 1, n in out)
            cross_next()
            work()
        while crossing:
            cross_next()
        while todo:
            work()

    def wo_first():
        SO.send(d, o_ring(1, 0, 0), onward)
        SO.wait(O_THEIRS)
        SO.send(theirs, o_ring(1, 1, 0), onward)
        SO.wait(O_Y)
        SO.send(other, o_ring(1, 0, 1), onward)
        SO.send(other, O_BOTH, sib)
        SO.wait(O_BOTH)
        SO.send(both, o_ring(1, 1, 1), onward)

    def wo_step(s):
        zo = zat_(-sgn * s)
        for n in (0,) if s == half else (0, 1):
            for r, yy in enumerate((yl, yo)):
                io = dpi(yy, zo, core_of(n))
                SO.wait(o_ring(s, n, r))
                if s < half - 1 or (s == half - 1 and n == 0):
                    SO.send(io, o_ring(s + 1, n, r), onward)
                SO.send(io, O_SIB, sib)

    def norm_rows(i, _):
        rr = pl.ds(pl.multiple_of(i * 32, 32), 32)
        x = hid[rr, :].astype(F32)
        ms = jnp.sum(x * x, axis=1, keepdims=True) * (1.0 / D)
        hid[rr, :] = (x * lax.rsqrt(ms + epsilon)).astype(BF16)
        return 0

    def rows_of(zz):
        return [pl.ds(pl.multiple_of(dpi(yy, zz, 0) * R, 2 * R), 2 * R) for yy in (0, 1)]

    def mm_q(zz):
        lhs = jnp.concatenate([hid[:, r] for r in rows_of(zz)], axis=1)
        rhs = jnp.concatenate([wq[r, :] for r in rows_of(zz)], axis=0)
        accq[...] += jnp.dot(lhs, rhs, preferred_element_type=F32)

    def mm_kv(zz):
        lhs = jnp.concatenate([hid[:, r] for r in rows_of(zz)], axis=1)
        rhs = jnp.concatenate([wkv[r, :] for r in rows_of(zz)], axis=0)
        acckv[...] += jnp.dot(lhs, rhs, preferred_element_type=F32)

    def opp_q(k):
        SQ.wait(q_sib(k), 8)
        mm_q(zat_(sgn * k))

    def opp_kv(k):
        SKV.wait(kv_sib(k - 1), 4)
        mm_kv(zat_(sgn * k))

    NB = 64

    def block_of(r):
        sub = r * NB + lax.broadcasted_iota(jnp.int32, (NB, 1), 0)
        posc = base + sub.astype(F32)
        epc = jnp.sum(jnp.where(rows_s[pl.ds(6, 1), pl.ds(0, nl)] <= posc, 1.0, 0.0), axis=1, keepdims=True)
        ll = lax.broadcasted_iota(jnp.int32, (NB, T), 1)
        ss = r * NB + lax.broadcasted_iota(jnp.int32, (NB, T), 0)
        return sub, epc, ll, ss

    def bias_rows(r, _):
        sub, epc, ll, ss = block_of(r)
        same = rows_s[pl.ds(0, 1), :] == epc
        bias[pl.ds(pl.multiple_of(r * NB, NB), NB), :] = jnp.where((ll <= ss) & same, 0.0, -1e30)
        return 0

    def angle_rows(r, _):
        n = 32
        rr = lax.broadcasted_iota(jnp.int32, (n, HEAD), 0)
        upper = jnp.where(lax.broadcasted_iota(jnp.int32, (n, HEAD), 1) < HEAD // 2, 0, T // 2)
        angles = (rr + upper + (d * T + r * n)).astype(F32) * jnp.concatenate([fr_ref[...], fr_ref[...]], axis=1)
        at = pl.ds(pl.multiple_of(r * n, n), n)
        cs_ref[at, :] = jnp.cos(angles)
        sn_ref[at, :] = jnp.sin(angles)
        return 0

    def gae_send():
        for k in range(1, nwin):
            pltpu.make_async_remote_copy(
                gae.at[0], gae.at[k], ssem.at[4], rmisc.at[0],
                device_id=dev(lax.rem(d + ndp - k, ndp), m), device_id_type=MESH,
            ).start()

    def advantages():
        landed(gae, 4, rmisc.at[0], nwin - 1)
        si, li, ends_col = ends()
        term_col = jnp.sum(jnp.where(li == si, term_ref[...].astype(F32), 0.0), axis=1, keepdims=True)
        for k in range(nwin):
            pos = base + (lane + k * T).astype(F32)
            ep = jnp.sum(jnp.where(ends_col <= pos, 1.0, 0.0), axis=0, keepdims=True)
            hit = (ends_col - 1.0) == pos
            fin = jnp.sum(jnp.where(hit, 1.0, 0.0), axis=0, keepdims=True)
            stp = jnp.sum(jnp.where(hit, term_col, 0.0), axis=0, keepdims=True)
            rew = gae[k, pl.ds(0, 1), :]
            old = gae[k, pl.ds(1, 1), :]
            nxt = pltpu.roll(old, T - 1, 1)
            if k + 1 < nwin:
                nxt = jnp.where(lane == T - 1, gae[k + 1, pl.ds(1, 1), :][:, :1], nxt)
            booted = jnp.where(fin > 0.0, (1.0 - stp) * old, nxt)
            delta = rew + discount * booted - old
            rows_s[pl.ds(k, 1), :] = ep
            rows_s[pl.ds(8 + k, 1), :] = delta * jnp.exp((lane + k * T).astype(F32) * kappa)

    def advantages_sum():
        def rowblock(r, advr):
            sub, epc, ll, ss = block_of(r)
            same = rows_s[pl.ds(0, 1), :] == epc
            tot = jnp.where((ll >= ss) & same, rows_s[pl.ds(8, 1), :], 0.0)
            for k in range(1, nwin):
                tot += jnp.where(rows_s[pl.ds(k, 1), :] == epc, rows_s[pl.ds(8 + k, 1), :], 0.0)
            col = jnp.sum(tot, axis=1, keepdims=True) * jnp.exp(sub.astype(F32) * (-kappa))
            return advr + jnp.sum(jnp.where(ll == ss, col, 0.0), axis=0, keepdims=True)

        adv_ref[...] = lax.fori_loop(0, T // NB, rowblock, jnp.zeros((1, T), F32))
        outs[0].start()

    SKV.send(d, KV_Y, ypart)
    for i in (0, 1):
        SQ.send(2 * d + i, Q_THEIRS, sib)
    SKV.send(d, KV_THEIRS, sib)
    for i in (0, 1):
        SQ.send(2 * d + i, q_ring(1, 0, i), onward)
    SKV.send(d, kv_ring(1, 0, 0), onward)
    for i in (0, 1):
        SQ.send(2 * d + i, q_cross(0, 0, i), ypart)
    SQ.wait(Q_THEIRS, 2)
    for i in (0, 1):
        SQ.send(2 * theirs + i, q_ring(1, 1, i), onward)
    SKV.wait(KV_THEIRS)
    SKV.send(theirs, kv_ring(1, 1, 0), onward)
    accq[...] = jnp.zeros_like(accq)
    acckv[...] = jnp.zeros_like(acckv)
    for copy in small + copies[4:5]:
        copy.wait()
    gae[0, pl.ds(0, 1), :] = rew_ref[...]
    gae[0, pl.ds(1, 1), :] = old_ref[...]
    first_marks()
    lax.fori_loop(0, 4, norm_rows, 0)
    def norms(lo, hi):
        return functools.partial(lax.fori_loop, lo, hi, norm_rows, 0)

    def other_kv():
        SKV.wait(KV_Y)
        SKV.send(other, kv_ring(1, 0, 1), onward)
        SKV.send(other, KV_BOTH, sib)

    def both_kv():
        SKV.wait(KV_BOTH)
        SKV.send(both, kv_ring(1, 1, 1), onward)

    qkv_step(1, [norms(4, 5), other_kv, both_kv, norms(5, 6), norms(6, 7), norms(7, 8), norms(8, 9), norms(9, 10)])
    def biases(lo, hi):
        return functools.partial(lax.fori_loop, lo, hi, bias_rows, 0)

    def own_q():
        SQ.wait(q_sib(0), 2)
        mm_q(z)

    def own_kv():
        mm_kv(z)

    qkv_step(2, [norms(10, 11), norms(11, 12), norms(12, 13), norms(13, 14), norms(14, 15), norms(15, 16), own_kv, own_q])
    def pieces_at(s):
        k = s - 2
        zm = zat_(-sgn * k)
        return [nothing, lambda: mm_q(zm), nothing, lambda: mm_kv(zm), nothing, lambda: opp_q(k), nothing, lambda: opp_kv(k)]

    share = T // NB // (half - 4)

    def mid(s, _):
        extra = pieces_at(s)
        extra[0] = functools.partial(lax.fori_loop, (s - 3) * share, (s - 2) * share, bias_rows, 0)
        extra[2] = lambda: angle_rows((s - 3) * 2, 0)
        extra[4] = lambda: angle_rows((s - 3) * 2 + 1, 0)
        qkv_step(s, extra)
        return 0

    lax.fori_loop(3, half - 1, mid, 0)
    copies[3].wait()
    SO.send(d, O_THEIRS, sib)
    SO.send(d, O_Y, ypart)
    qkv_step(half - 1, pieces_at(half - 1), out=(0,))
    wo_first()
    qkv_step(half, pieces_at(half), cores=(0,), out=())
    mm_kv(zat_(-sgn * (half - 1)))
    mm_q(zat_(-sgn * (half - 1)))
    for i in (0, 1):
        across(half, 0, i)
    opp_kv(half - 1)
    opp_q(half - 1)
    SKV.wait(kv_sib(half - 1), 2)
    mm_kv(zat_(half))
    wo_step(1)
    SQ.wait(q_sib(half), 4)
    mm_q(zat_(half))

    low = lax.broadcasted_iota(jnp.int32, (T // 2, HEAD), 1) < HEAD // 2

    def spread(ref, sign):
        table = ref[...]
        turned = pltpu.roll(table, HEAD // 2, 1)
        first, second = jnp.where(low, table, turned), jnp.where(low, turned, table)
        if sign:
            first, second = jnp.where(low, -first, first), jnp.where(low, -second, second)
        return first, second

    cosines, sines = spread(cs_ref, False), spread(sn_ref, True)

    def rope(load, store):
        for n in (0, 1):
            x = load(slice(n * T // 2, (n + 1) * T // 2))
            store(slice(n * T // 2, (n + 1) * T // 2), (x * cosines[n] + pltpu.roll(x, HEAD // 2, 1) * sines[n]).astype(BF16))

    def put_q(h):
        def store(r, x):
            qs[h, r, :] = x
        return store

    def put_k(r, x):
        ks[r, :] = x

    def rope_q(h):
        rope(lambda r: accq[r, h * HEAD:(h + 1) * HEAD], put_q(h))

    rope(lambda r: acckv[r, :FK], put_k)
    vs[...] = acckv[:, FK:].astype(BF16)

    scale = 1.0 / HEAD**0.5

    number, bulk = att_numbers(heads)

    def att_copy(o, p, kind, k, to):
        i = o * (2 * heads) + p
        n = number(kind, k, p)
        return pltpu.make_async_remote_copy(
            att.at[i], att.at[i], ssem.at[3], ratt.at[n], device_id=to, device_id_type=MESH
        )

    def att_send(o, p, kind, k, to):
        att_copy(o, p, kind, k, to).start()

    def att_wait(o, p, kind, k):
        if number(kind, k, p) >= len(bulk):
            att_copy(o, p, kind, k, sib).wait_recv()

    def att_rest(n):
        landed(att, 3, ratt.at[n], bulk[n])

    QB = 128

    def piece_send(p):
        att_send(m, p, "near", -1, xdev(away(p)))
        att_send(m, p, "near", 1, xdev(away(p, -1)))
        att_send(m, p, "y", 0, yx)

    def head_step(h):
        for i in range(T // QB):
            n = (i + 1) * QB
            sc = lax.dot_general(
                qs[h, i * QB:n, :], ks[:n, :], (((1,), (1,)), ((), ())), preferred_element_type=F32
            ) * scale + bias[i * QB:n, :n]
            big = jnp.max(sc, axis=1, keepdims=True)
            ex = jnp.exp(sc - big)
            pr = (ex / jnp.sum(ex, axis=1, keepdims=True)).astype(BF16)
            out = jnp.dot(pr, vs[:n, :], preferred_element_type=F32)
            r = 2 * i // (T // QB)
            low_row = i * QB - r * (T // 2)
            att[m * (2 * heads) + 2 * h + r, low_row:low_row + QB, :] = out.astype(BF16)
            if (i + 1) * 2 % (T // QB) == 0:
                piece_send(2 * h + r)

    rope_q(0)
    head_step(0)
    rope_q(1)
    head_step(1)
    gae_send()
    wo_step(2)
    rope_q(2)
    head_step(2)
    for h in range(3, heads):
        rope_q(h)
        head_step(h)

    cut = CUT

    def relay_near(p):
        for k in (-1, 1):
            o = mpi(yh, away(p, k))
            att_wait(o, p, "near", k)
            if k == -1:
                att_send(o, p, "two", 0, xdev(away(p)))
            if p < cut:
                att_send(o, p, "far", k, yx)

    def relay_two(p):
        o = mpi(yh, 2)
        att_wait(o, p, "two", 0)
        if p < cut:
            att_send(o, p, "last", 0, yx)

    def relay_y(p):
        o = mpi(1 - yh, 0)
        att_wait(o, p, "y", 0)
        if p >= cut:
            att_send(o, p, "far", -1, xdev(away(p)))
            att_send(o, p, "far", 1, xdev(away(p, -1)))

    def relay_far(p):
        for k in (-1, 1):
            o = mpi(1 - yh, away(p, k))
            att_wait(o, p, "far", k)
            if p >= cut and k == -1:
                att_send(o, p, "last", 0, xdev(away(p)))

    for p in range(cut):
        relay_near(p)
    wo_step(3)
    advantages()
    wo_step(4)
    advantages_sum()
    for p in range(cut, 2 * heads):
        relay_near(p)
        relay_y(p)
    wo_step(5)
    for p in range(cut):
        relay_two(p)
    wo_step(6)
    relay_far(3)
    relay_far(4)
    wo_step(7)
    relay_far(5)
    relay_far(6)
    relay_far(7)
    wo_step(8)

    SO.wait(O_SIB, 4 * half - 2)
    def project(o):
        r0 = pl.ds(pl.multiple_of(o * FQ, FQ), FQ)
        for r in (0, 1):
            lhs = jnp.concatenate([att[o * (2 * heads) + 2 * h + r] for h in range(heads)], axis=1)
            acco[r * T // 2:(r + 1) * T // 2, :] += jnp.dot(lhs, wo[r0, :], preferred_element_type=F32)

    copies[5].wait()
    acco[...] = hown[...].astype(F32)
    project(m)
    att_rest(0)
    project(mpi(yh, 1))
    project(mpi(yh, -1))
    att_rest(1)
    project(mpi(yh, 2))
    att_rest(2)
    project(mpi(1 - yh, 0))
    att_rest(3)
    project(mpi(1 - yh, 1))
    project(mpi(1 - yh, -1))
    att_rest(4)
    project(mpi(1 - yh, 2))

    def sums(r, carry):
        n = 64
        x = acco[pl.ds(pl.multiple_of(r * n, n), n), :]
        ll = lax.broadcasted_iota(jnp.int32, (n, T), 1)
        ss = r * n + lax.broadcasted_iota(jnp.int32, (n, T), 0)
        sq = jnp.sum(x * x, axis=1, keepdims=True)
        hs = jnp.sum(x * vw_ref[...], axis=1, keepdims=True)
        a, b = carry
        a = a + jnp.sum(jnp.where(ll == ss, sq, 0.0), axis=0, keepdims=True)
        b = b + jnp.sum(jnp.where(ll == ss, hs, 0.0), axis=0, keepdims=True)
        return a, b

    zero = jnp.zeros((1, T), F32)
    sq, hs = lax.fori_loop(0, T // 64, sums, (zero, zero), unroll=True)
    red[m, pl.ds(0, 1), :] = sq
    red[m, pl.ds(1, 1), :] = hs
    for mm in mpeers:
        pltpu.make_async_remote_copy(
            red.at[m], red.at[m], ssem.at[5], rmisc.at[1], device_id=dev(d, mm), device_id_type=MESH
        ).start()
    landed(red, 5, rmisc.at[1], 2 * nx - 1)
    tot = red[0]
    for k in range(1, 2 * nx):
        tot = tot + red[k]
    value = tot[1:2] * lax.rsqrt(tot[0:1] * (1.0 / D) + epsilon)
    val_ref[...] = value
    outs[1].start()
    old = old_ref[...]
    returns = adv_ref[...] + old
    clipped = old + jnp.clip(value - old, -clip_range, clip_range)
    terms = jnp.maximum((value - returns) ** 2, (clipped - returns) ** 2)
    part = jnp.sum(terms, axis=1, keepdims=True)

    lz[d] = jnp.broadcast_to(part, lz.shape[1:])
    far = sorted(range(nz), key=lambda k: -min(k, nz - k))
    for k in far:
        for yy in (yo, yl):
            for cc in (co, c):
                if k == 0 and yy is yl and cc is c:
                    continue
                pltpu.make_async_remote_copy(
                    lz.at[d], lz.at[d], ssem.at[6], rmisc.at[2],
                    device_id=dev(dpi(yy, zat(k), cc), m), device_id_type=MESH,
                ).start()

    landed(lz, 6, rmisc.at[2], ndp - 1)
    total = lz[0]
    for k in range(1, ndp):
        total = total + lz[k]
    loss_ref[...] = total * (0.5 / (T * ndp))
    outs[2].start()

    SQ.drain(2 * (ndp - 1))
    SKV.drain(ndp - 1)
    SO.drain(ndp - 1)

    def drain(buf, sem, count):
        ref = buf.at[pl.ds(0, count)]
        pltpu.make_async_remote_copy(
            ref, ref, ssem.at[sem], rmisc.at[1], device_id=sib, device_id_type=MESH
        ).wait_send()

    drain(att, 3, 14 * heads)
    drain(gae, 4, nwin - 1)
    drain(red, 5, 2 * nx - 1)
    drain(lz, 6, ndp - 1)
    for copy in outs:
        copy.wait()


def solution(mesh):
    ndp, nmp = mesh.shape["dp"], mesh.shape["mp"]
    nz, nx = ndp // 4, nmp // 2
    nwin = 5

    def body(hidden_in, w_query, w_key, w_value, w_out, value_weight, rewards, old_values, lengths, terminal):
        T, D = hidden_in.shape
        R, FQ = w_query.shape
        FK = w_key.shape[1]
        heads = FQ // HEAD
        nl = lengths.shape[0]
        half = HEAD // 2
        freq = np.power(rope_base, -np.arange(half, dtype=np.float64) * 2.0 / HEAD).astype(np.float32)
        any_ = pl.BlockSpec(memory_space=pl.ANY)
        dma = pltpu.SemaphoreType.DMA
        out, loss = pl.pallas_call(
            functools.partial(kernel, nz, nx),
            out_shape=(
                jax.ShapeDtypeStruct((2, 1, T), F32),
                jax.ShapeDtypeStruct((1, 128), F32),
            ),
            in_specs=[any_] * 11,
            out_specs=(any_, any_),
            scratch_shapes=[
                pltpu.VMEM((T // 2, HEAD), F32),
                pltpu.VMEM((T // 2, HEAD), F32),
                pltpu.VMEM((1, HEAD // 2), F32),
                pltpu.VMEM((1, FQ), F32),
                pltpu.VMEM((1, T), F32),
                pltpu.VMEM((1, T), F32),
                pltpu.VMEM((1, nl), jnp.int32),
                pltpu.VMEM((1, nl), jnp.int32),
                pltpu.VMEM((1, T), F32),
                pltpu.VMEM((1, T), F32),
                pltpu.VMEM((1, 128), F32),
                pltpu.VMEM((T, D), BF16),
                pltpu.VMEM((T, FQ), BF16),
                pltpu.VMEM((D, FQ), BF16),
                pltpu.VMEM((D, 2 * FK), BF16),
                pltpu.VMEM((D, FQ), BF16),
                pltpu.VMEM((nmp * 2 * heads, T // 2, HEAD), BF16),
                pltpu.VMEM((T, FQ), F32),
                pltpu.VMEM((T, 2 * FK), F32),
                pltpu.VMEM((heads, T, HEAD), BF16),
                pltpu.VMEM((T, HEAD), BF16),
                pltpu.VMEM((T, HEAD), BF16),
                pltpu.VMEM((T, T), F32),
                pltpu.VMEM((T, FQ), F32),
                pltpu.VMEM((16, T), F32),
                pltpu.VMEM((nwin, 2, T), F32),
                pltpu.VMEM((nmp, 2, T), F32),
                pltpu.VMEM((ndp, 1, 128), F32),
                dma((15,)),
                dma((9 * nz // 2 + 2,)),
                dma((5 * nz // 2 + 2,)),
                dma((2 * nz + 2,)),
                dma((att_sems(heads),)),
                dma((3,)),
                dma((7,)),
            ],
            compiler_params=pltpu.CompilerParams(collective_id=0, has_side_effects=True),
        )(
            hidden_in, w_query, w_key, w_value, w_out, jnp.asarray(freq.reshape(1, half)),
            value_weight.reshape(1, FQ), rewards.reshape(1, T), old_values.reshape(1, T),
            lengths.reshape(1, nl), terminal.reshape(1, nl),
        )
        return out[0, 0], out[1, 0], loss[0, 0]

    return jax.shard_map(
        body,
        mesh=mesh,
        in_specs=(
            P("dp", None), P("dp", "mp"), P("dp", "mp"), P("dp", "mp"), P("dp", "mp"),
            P("mp"), P("dp"), P("dp"), P(), P(),
        ),
        out_specs=(P("dp"), P("dp"), P()),
        check_vma=False,
    )
```
